256 devices in a mesh: groups: 4 (over y, x), seq: 32 (over z), batch: 2 (over core).
Axes of the slice: x: 2, y: 2, z: 32, core: 2. Of those that a mesh axis runs over, the one named last changes fastest.
The devices are a block of a 4x8x32 slice.
Arguments:
- prompt_cache: bfloat16 [32, 1024, 8, 256], P(('groups', 'batch'), 'seq'), parts along dimension 0, may hold values from -6 to 6
- prompt_states: float32 [32, 32, 16, 16384], P(('groups', 'batch'), 'seq'), parts along dimension 0, may hold values from -6 to 6
- block_steps: float32 [32, 32, 16384], P(('groups', 'batch'), 'seq'), parts along dimension 0, may hold values from 0.005 to 0.1
- prompt_lengths: int32 [32], P('groups'), parts along dimension 0, may hold values from 170 to 1023
- target_slots: int32 [32], P('groups'), parts along dimension 0, may hold values from 0 to 15, as said below
- cache_lengths: int32 [64], P(('groups', 'batch')), parts along dimension 0, may hold values from 170 to 1023
- resident_cache: bfloat16 [64, 32, 32, 8, 256], P(('groups', 'batch'), None, 'seq'), parts along dimension 0, may hold values from -6 to 6
- token_cache: bfloat16 [64, 8, 256], P(('groups', 'batch')), parts along dimension 0, may hold values from -6 to 6
- queries: bfloat16 [64, 64, 128], P(('groups', 'batch')), parts along dimension 0, may hold values from -6 to 6
- resident_states: float32 [64, 16, 16384], P(('groups', 'batch'), None, 'seq'), parts along dimension 0, may hold values from -6 to 6
- decay_rates: float32 [16, 16384], replicated, may hold values from 0.05 to 10
- step_sizes: float32 [64, 16384], P(('groups', 'batch'), 'seq'), parts along dimension 0, may hold values from 0.01 to 1
- inner_input: bfloat16 [64, 16384], P(('groups', 'batch'), 'seq'), parts along dimension 0, may hold values from -6 to 6
- inner_gate: bfloat16 [64, 16384], P(('groups', 'batch'), 'seq'), parts along dimension 0, may hold values from -6 to 6
- state_input: float32 [64, 16], P(('groups', 'batch')), parts along dimension 0, may hold values from -6 to 6
- state_readout: float32 [64, 16], P(('groups', 'batch')), parts along dimension 0, may hold values from -6 to 6
- skip_gain: float32 [16384], P('seq'), may hold values from 0.5 to 1.5
Outputs:
- merged_cache: bfloat16 [64, 32, 32, 8, 256], P(('groups', 'batch'), None, 'seq'), parts along dimension 0
- attention: bfloat16 [64, 64, 128], P(('groups', 'batch'), 'seq'), parts along dimension 0
- next_states: float32 [64, 16, 16384], P(('groups', 'batch'), None, 'seq'), parts along dimension 0
- mamba_output: bfloat16 [64, 16384], P(('groups', 'batch'), 'seq'), parts along dimension 0
The draws below stay inside these ranges and needn't reach their ends.
There are 4 independent parts, one for each index of `groups`. The reference program is written for one: setup_inputs(seed, part) draws one part's arguments, and reference() takes and returns one part's arrays. A program takes and returns all parts, laid end to end along the dimension named above; an argument that names none is the same for every part. Nothing has to cross between parts.
Inputs may be any that keep to these rules, and one draw needn't show every extreme that they name: `target_slots`: 8 distinct slots.
All inputs are finite; a program needn't handle non-finite values.
Results may differ from the reference program's by a relative error of at most 0.0019.
Values may be sent and summed in bfloat16 or wider, within the bound.
No kernel may reach another device: no remote copies, remote signals or barrier semaphores. Data moves between devices by JAX's collectives and lax.ppermute only.
A program may use at most 320 MiB of HBM per device.

```python
import math
import jax
import jax.numpy as jnp
from jax import lax

HEADS = 64
KV_HEADS = 8
HEAD_DIM = 128
INNER = 16384
STATE = 16
PROMPTS = 8
BLOCK_LEN = 32
SLOTS_DEV = 8
PROMPT_MAX = 1024
SLOTS = 16
N_SEQ = 32
N_BATCH = 2


def draw_target_slots(key, part):
    shuffled = jax.random.permutation(key, SLOTS)
    return shuffled[:PROMPTS].astype(jnp.int32)


def sign_direction(key):
    return jax.random.rademacher(jax.random.fold_in(key, 7101), (KV_HEADS, HEAD_DIM), dtype=jnp.float32)


def key_amplitudes():
    return jnp.array([4.8, 4.76, 4.72], jnp.float32)


def keyed_cache(key, row_count, salt_value, level_set):
    kv_width = 2 * HEAD_DIM
    noise_key, spot_key, fine_key = jax.random.split(jax.random.fold_in(key, salt_value), 3)
    base_draw = jnp.clip(jax.random.normal(noise_key, (row_count, PROMPT_MAX, KV_HEADS, kv_width), jnp.float32), -6.0, 6.0)
    reach_len = max(PROMPT_MAX // 6, 3)

    def pick_spots(row_index):
        return jax.random.permutation(jax.random.fold_in(spot_key, row_index), reach_len)[:3].astype(jnp.int32)
    spot_rows = jax.vmap(pick_spots)(jnp.arange(row_count, dtype=jnp.int32))
    position = jnp.arange(PROMPT_MAX, dtype=jnp.int32)
    hit_table = (position[None, None, :] == spot_rows[:, :, None]).astype(jnp.float32)
    amplitude = jnp.einsum('rkt,k->rt', hit_table, level_set)
    chosen = jnp.sum(hit_table, axis=1)
    direction = sign_direction(key)
    fine_noise = 0.02 * jnp.clip(jax.random.normal(fine_key, (row_count, PROMPT_MAX, KV_HEADS, HEAD_DIM), jnp.float32), -3.0, 3.0)
    aligned = amplitude[:, :, None, None] * direction[None, None] + fine_noise
    new_keys = jnp.where(chosen[:, :, None, None] > 0.5, aligned, base_draw[..., :HEAD_DIM])
    return jnp.concatenate([new_keys, base_draw[..., HEAD_DIM:]], axis=3)


def draw_prompt_cache(key, part):
    level_set = key_amplitudes()
    return keyed_cache(key, PROMPTS, 11, level_set).astype(jnp.bfloat16)


def draw_resident_cache(key, part):
    level_set = key_amplitudes()
    filled = keyed_cache(key, SLOTS, 13, level_set)
    return filled.reshape(SLOTS, BLOCK_LEN, -1, KV_HEADS, 2 * HEAD_DIM).astype(jnp.bfloat16)


def draw_queries(key, part):
    group_size = HEADS // KV_HEADS
    direction = sign_direction(key)
    head_dirs = jnp.repeat(direction, group_size, axis=0)
    mask_key, level_key, noise_key, fine_key = jax.random.split(jax.random.fold_in(key, 17), 4)
    drawn = jnp.clip(jax.random.normal(noise_key, (SLOTS, HEADS, HEAD_DIM), jnp.float32), -6.0, 6.0)
    picked = jax.random.bernoulli(mask_key, 0.25, (SLOTS, HEADS))
    strength = jax.random.uniform(level_key, (SLOTS, HEADS), jnp.float32, 2.2, 5.5)
    fine_noise = 0.1 * jnp.clip(jax.random.normal(fine_key, (SLOTS, HEADS, HEAD_DIM), jnp.float32), -3.0, 3.0)
    aligned = jnp.clip(strength[..., None] * head_dirs[None] + fine_noise, -6.0, 6.0)
    return jnp.where(picked[..., None], aligned, drawn).astype(jnp.bfloat16)


def set_ends(result, key, least, top_value):
    place = [jax.random.randint(jax.random.fold_in(key, axis), (), 0, length) for axis, length in enumerate(result.shape)]
    longest = result.shape.index(max(result.shape))
    neighbour = place[:longest] + [(place[longest] + 1) % result.shape[longest]] + place[longest + 1:]
    return result.at[tuple(place)].set(least).at[tuple(neighbour)].set(top_value)


def strengthened(drawn, own_key, source, target, parts, factor):
    def block_of(axis_at):
        return (jnp.arange(drawn.shape[axis_at]) // (drawn.shape[axis_at] // parts)).reshape((-1,) + (1,) * (drawn.ndim - 1 - axis_at))

    near = jax.random.permutation(own_key, parts)[block_of(target)]
    other_side = (block_of(target) + parts // 2) % parts
    return jnp.where((block_of(source) == near) | (block_of(source) == other_side), factor * drawn, drawn)


def block_scale(stream_key, extent, pieces, least, top_value):
    def one(dim, parts):
        draws = jax.random.uniform(jax.random.fold_in(jax.random.fold_in(stream_key, 6), dim), (parts,), jnp.float32, least / len(pieces), top_value / len(pieces))
        return jnp.repeat(jnp.exp(draws), extent[dim] // parts).reshape((-1,) + (1,) * (len(extent) - dim - 1))

    level = one(*pieces[0])
    for cut in pieces[1:]:
        level = level * one(*cut)
    return level


def gaussian(key, extent, width, reach, shards=(), held_as=jnp.bfloat16):
    drawn = jax.random.normal(key, extent, jnp.float32) * width
    if len(shards) > 0:
        drawn = block_scale(key, extent, shards, -0.22, 0.18) * drawn
    return jnp.clip(drawn, min=-reach, max=reach).astype(held_as)


def heavy_noise(own_key, extent, spread, bound, cuts, heavy, held_as=jnp.bfloat16):
    values = spread * jax.random.normal(own_key, extent, jnp.float32)
    if cuts:
        values = values * block_scale(own_key, extent, cuts, -0.22, 0.18)
    return jnp.clip(strengthened(values, jax.random.fold_in(own_key, 3), *heavy), -bound, bound).astype(held_as)


def setup_inputs(seed: int = 0, part: int = 0) -> dict:
    key_list = jax.random.split(jax.random.key(seed), 18)
    part_keys = jax.random.split(jax.random.fold_in(key_list[17], part), 18)
    prompt_cache = draw_prompt_cache(jax.random.fold_in(jax.random.fold_in(key_list[17], part), 71), part)
    prompt_states = heavy_noise(part_keys[1], (PROMPTS, N_SEQ, STATE, INNER), 1.0, 6.0, ((0, 2), (1, 32)), (1, 3, 32, 2.75), jnp.float32)
    block_steps = jnp.clip(jnp.exp(math.log(0.1) - 2.9957323 * jax.random.uniform(part_keys[2], (PROMPTS, N_SEQ, INNER), jnp.float32) ** block_scale(part_keys[2], (PROMPTS, N_SEQ, INNER), ((0, 2), (1, 32)), -0.2, 0.2)), 0.005, 0.1)
    prompt_lengths = set_ends(jax.random.randint(part_keys[3], (PROMPTS,), PROMPT_MAX // 6, PROMPT_MAX), jax.random.fold_in(part_keys[3], 1), PROMPT_MAX // 6, PROMPT_MAX - 1).astype(jnp.int32)
    target_slots = draw_target_slots(jax.random.fold_in(jax.random.fold_in(key_list[17], part), 71), part)
    cache_lengths = set_ends(jax.random.randint(part_keys[5], (SLOTS,), PROMPT_MAX // 6, PROMPT_MAX), jax.random.fold_in(part_keys[5], 1), PROMPT_MAX // 6, PROMPT_MAX - 1).astype(jnp.int32)
    resident_cache = draw_resident_cache(jax.random.fold_in(jax.random.fold_in(key_list[17], part), 71), part)
    token_cache = gaussian(part_keys[7], (SLOTS, KV_HEADS, 2 * HEAD_DIM), 1.0, 6.0, ((0, 2),))
    queries = draw_queries(jax.random.fold_in(jax.random.fold_in(key_list[17], part), 71), part)
    resident_states = gaussian(part_keys[9], (SLOTS, STATE, INNER), 1.0, 6.0, ((0, 2), (2, 32)), jnp.float32)
    decay_rates = jnp.clip(jnp.exp(jax.random.uniform(key_list[10], (STATE, INNER), jnp.float32, math.log(0.05), math.log(10.0))), 0.05, 10.0)
    step_sizes = jnp.clip(jnp.exp(math.log(1.0) - 4.6051702 * jax.random.uniform(part_keys[11], (SLOTS, INNER), jnp.float32) ** block_scale(part_keys[11], (SLOTS, INNER), ((0, 2), (1, 32)), -0.2, 0.2)), 0.01, 1.0)
    inner_input = gaussian(part_keys[12], (SLOTS, INNER), 1.0, 6.0, ((0, 2), (1, 32)))
    inner_gate = gaussian(part_keys[13], (SLOTS, INNER), 1.0, 6.0, ((0, 2), (1, 32)))
    state_input = gaussian(part_keys[14], (SLOTS, STATE), 1.0, 6.0, ((0, 2),), jnp.float32)
    state_readout = gaussian(part_keys[15], (SLOTS, STATE), 1.0, 6.0, ((0, 2),), jnp.float32)
    skip_gain = jnp.clip(0.5 + 1.0 * jax.random.uniform(key_list[16], (INNER,), jnp.float32) ** block_scale(key_list[16], (INNER,), ((0, 32),), -0.2, 0.2), 0.5, 1.5)
    return {"prompt_cache": prompt_cache, "prompt_states": prompt_states, "block_steps": block_steps, "prompt_lengths": prompt_lengths, "target_slots": target_slots, "cache_lengths": cache_lengths, "resident_cache": resident_cache, "token_cache": token_cache, "queries": queries, "resident_states": resident_states, "decay_rates": decay_rates, "step_sizes": step_sizes, "inner_input": inner_input, "inner_gate": inner_gate, "state_input": state_input, "state_readout": state_readout, "skip_gain": skip_gain}


def reference(prompt_cache, prompt_states, block_steps, prompt_lengths, target_slots, cache_lengths, resident_cache, token_cache, queries, resident_states, decay_rates, step_sizes, inner_input, inner_gate, state_input, state_readout, skip_gain):
    prompt_max = BLOCK_LEN * N_SEQ
    slot_count = SLOTS_DEV * N_BATCH
    kv_width = 2 * HEAD_DIM
    slot_ids = jnp.arange(slot_count, dtype=jnp.int32)
    matches = target_slots[None, :] == slot_ids[:, None]
    fresh = jnp.any(matches, axis=1)
    chosen_len = lax.optimization_barrier(jnp.sum(jnp.where(matches, prompt_lengths[None, :], 0), axis=1)).astype(jnp.int32)
    lengths = jnp.where(fresh, chosen_len, cache_lengths).astype(jnp.int32)
    picked = jnp.dot(matches.astype(jnp.bfloat16), prompt_cache.reshape(PROMPTS, -1), preferred_element_type=jnp.float32)
    picked = picked.astype(jnp.bfloat16).reshape(slot_count, prompt_max, KV_HEADS, kv_width)
    resident = resident_cache.reshape(slot_count, prompt_max, KV_HEADS, kv_width)
    position = jnp.arange(prompt_max, dtype=jnp.int32)
    merged = jnp.where(fresh[:, None, None, None], picked, resident)
    merged = jnp.where((position[None, :] < lengths[:, None])[:, :, None, None], merged, jnp.zeros((), jnp.bfloat16))
    merged = jnp.where((position[None, :] == lengths[:, None])[:, :, None, None], token_cache[:, None], merged)
    merged_cache = merged.reshape(slot_count, BLOCK_LEN, N_SEQ, KV_HEADS, kv_width)
    group = HEADS // KV_HEADS
    grouped = queries.reshape(slot_count, KV_HEADS, group, HEAD_DIM).astype(jnp.float32)
    scores = jnp.einsum('rgqd,rtgd->rgqt', grouped, merged[..., :HEAD_DIM].astype(jnp.float32)) * (1.0 / math.sqrt(HEAD_DIM))
    seen = (position[None, :] <= lengths[:, None])[:, None, None, :]
    masked = jnp.where(seen, scores, -1e+30)
    masked = masked.reshape(slot_count, KV_HEADS, group, BLOCK_LEN, N_SEQ)
    seen_cls = jnp.broadcast_to(seen, scores.shape).reshape(slot_count, KV_HEADS, group, BLOCK_LEN, N_SEQ)
    class_top = lax.optimization_barrier(jnp.max(masked, axis=3))
    weights = jnp.where(seen_cls, jnp.exp(masked - class_top[:, :, :, None, :]), 0.0)
    class_total = lax.optimization_barrier(jnp.sum(weights, axis=3))
    values = merged_cache[..., HEAD_DIM:].astype(jnp.float32)
    class_sum = jnp.einsum('rgqij,rijgd->rgqjd', weights.astype(jnp.bfloat16).astype(jnp.float32), values)
    overall = lax.optimization_barrier(jnp.max(class_top, axis=3))
    factor = jnp.exp(class_top - overall[..., None])
    total = lax.optimization_barrier(jnp.sum(class_total * factor, axis=3))
    summed = lax.optimization_barrier(jnp.sum(class_sum * factor[..., None], axis=3))
    attention = (summed / total[..., None]).reshape(slot_count, HEADS, HEAD_DIM).astype(jnp.bfloat16)
    starts = jnp.arange(N_SEQ, dtype=jnp.int32) * BLOCK_LEN
    usable = (starts[None, :] < prompt_lengths[:, None]).astype(jnp.float32)
    step_terms = block_steps * usable[:, :, None]
    later = lax.optimization_barrier(jnp.sum(step_terms, axis=1, keepdims=True)) - jnp.cumsum(step_terms, axis=1)

    def fold_prompt(packed):
        states, behind, weight = packed
        return lax.optimization_barrier(jnp.sum(weight[:, None, None] * jnp.exp(-decay_rates[None] * behind[:, None, :]) * states, axis=0))
    handed = lax.map(fold_prompt, (prompt_states, later, usable))
    chosen_state = jnp.einsum('rp,pnc->rnc', matches.astype(jnp.float32), handed, precision=lax.Precision.HIGHEST)
    start = jnp.where(fresh[:, None, None], chosen_state, resident_states)
    inner = inner_input.astype(jnp.float32)
    next_states = jnp.exp(-decay_rates[None] * step_sizes[:, None, :]) * start + (step_sizes * inner)[:, None, :] * state_input[:, :, None]
    readout = lax.optimization_barrier(jnp.sum(state_readout[:, :, None] * next_states, axis=1)) + skip_gain[None, :] * inner
    mamba_output = (readout * jax.nn.silu(inner_gate.astype(jnp.float32))).astype(jnp.bfloat16)
    return (merged_cache, attention, next_states, mamba_output)
```

```python
import functools
import math

import jax
import jax.numpy as jnp
from jax import lax
from jax.experimental import pallas as pl
from jax.experimental.pallas import tpu as pltpu
from jax.sharding import PartitionSpec as P


STATE_SCALE = 128.0
HALF_SPLIT = 8193.0
KERNEL_VMEM = 8 * 1024 * 1024


def split_half(value):
    spread = value * HALF_SPLIT
    high = spread - (spread - value)
    return high, value - high


def hop_kernel(
    flags,
    usable,
    up_in,
    down_in,
    up_state,
    up_step,
    up_rate,
    down_state,
    down_step,
    down_rate,
    up_out,
    down_out,
    *,
    initial,
    with_down,
):
    count, state = up_state.shape[0], up_state.shape[1]
    rows = count * state
    first, last, frozen = flags[0] == 1, flags[1] == 1, flags[2] == 1

    @pl.loop(0, count)
    def _(p):
        here = pl.ds(pl.multiple_of(p * state, state), state)
        rest = pl.ds(pl.multiple_of(rows + p * state, state), state)
        there = pl.ds(pl.multiple_of(2 * rows + p * state, state), state)
        wide, narrow = pl.ds(3 * rows + p, 1), pl.ds(3 * rows + count + p, 1)
        use = usable[p]
        own = up_state[p] * (use * STATE_SCALE)
        step = up_step[pl.ds(p, 1), :] * use
        if initial:
            acc, aside, span = own, jnp.zeros_like(own), step
        else:
            came, kept = up_in[here, :] + up_in[rest, :], up_in[there, :]
            acc = jnp.exp(-up_rate[...] * step) * jnp.where(first, 0.0, came) + own
            aside = jnp.where(first, came, kept)
            span = up_in[wide, :] + up_in[narrow, :]
            span = jnp.where(frozen, span, span + step)
        up_out[here, :], up_out[rest, :] = split_half(acc)
        up_out[there, :] = aside
        up_out[wide, :], up_out[narrow, :] = split_half(span)
        if not with_down:
            return
        own = down_state[p] * (use * STATE_SCALE)
        step = down_step[pl.ds(p, 1), :] * use
        if initial:
            acc, aside, span = own, jnp.zeros_like(own), step
        else:
            came, kept = down_in[here, :] + down_in[rest, :], down_in[there, :]
            span = jnp.where(last, 0.0, down_in[wide, :] + down_in[narrow, :])
            acc = jnp.where(last, 0.0, came) + jnp.exp(-down_rate[...] * span) * own
            aside = jnp.where(last, came, kept)
            span = span + step
        down_out[here, :], down_out[rest, :] = split_half(acc)
        down_out[there, :] = aside
        down_out[wide, :], down_out[narrow, :] = split_half(span)


def last_kernel(
    flags, usable, up_in, down_in, own_state, own_step, own_rate, handed
):
    count, state = own_state.shape[0], own_state.shape[1]
    rows = count * state
    first, last, outside = flags[0] == 1, flags[1] == 1, flags[2] == 1
    rate = own_rate[...]

    @pl.loop(0, count)
    def _(p):
        here = pl.ds(pl.multiple_of(p * state, state), state)
        rest = pl.ds(pl.multiple_of(rows + p * state, state), state)
        there = pl.ds(pl.multiple_of(2 * rows + p * state, state), state)
        wide, narrow = pl.ds(3 * rows + p, 1), pl.ds(3 * rows + count + p, 1)
        use = usable[p]
        own = own_state[p] * (use * STATE_SCALE)
        step = own_step[pl.ds(p, 1), :] * use
        came, kept = up_in[here, :] + up_in[rest, :], up_in[there, :]
        newest = jnp.where(first, came, kept)
        earlier = jnp.where(first, 0.0, came)
        span = up_in[wide, :] + up_in[narrow, :]
        came, kept = down_in[here, :] + down_in[rest, :], down_in[there, :]
        oldest = jnp.where(last, came, kept)
        later = jnp.where(last, 0.0, came)
        span_down = jnp.where(last, 0.0, down_in[wide, :] + down_in[narrow, :])
        outer = jnp.where(outside, span, 0.0)
        inner = earlier + jnp.exp(-rate * span) * oldest
        inner = later + jnp.exp(-rate * span_down) * (own + jnp.exp(-rate * step) * inner)
        handed[p] = (newest + jnp.exp(-rate * outer) * inner) * (1.0 / STATE_SCALE)


def smem():
    return pl.BlockSpec(memory_space=pltpu.SMEM)


def vmem():
    return pl.BlockSpec(memory_space=pltpu.VMEM)


def hand_over(states, steps, rates, usable, seq_count, seq_index):
    count, state, channels = states.shape
    width = channels // seq_count
    half = seq_count // 2
    ahead = [(k, (k + 1) % seq_count) for k in range(seq_count)]
    behind = [(k, (k - 1) % seq_count) for k in range(seq_count)]
    rows = 3 * count * state + 2 * count
    payload = jax.ShapeDtypeStruct((rows, width), jnp.float32)

    def fetched(chunk):
        at = chunk * width
        return (
            lax.dynamic_slice_in_dim(states, at, width, 2),
            lax.dynamic_slice_in_dim(steps, at, width, 1),
            lax.dynamic_slice_in_dim(rates, at, width, 1),
        )

    def flags(third):
        return jnp.stack(
            [seq_index == 0, seq_index == seq_count - 1, third]
        ).astype(jnp.int32)

    cost = pl.CostEstimate(
        flops=16 * rows * width, bytes_accessed=16 * rows * width, transcendentals=rows * width
    )
    up = down = jnp.zeros((8, 128), jnp.float32)
    for hop in range(half):
        with jax.named_scope(f"ring_{hop}"):
            with_down = hop < half - 1
            ups = fetched((seq_index + half - hop) % seq_count)
            downs = fetched((seq_index - (half - 1) + hop) % seq_count) if with_down else ups
            operands = (flags(seq_index < hop), usable, up, down, *ups, *downs)
            outs = pl.pallas_call(
                functools.partial(hop_kernel, initial=hop == 0, with_down=with_down)
                if with_down
                else functools.partial(
                    lambda *refs, **kw: hop_kernel(*refs, None, **kw),
                    initial=hop == 0,
                    with_down=False,
                ),
                out_shape=(payload, payload) if with_down else (payload,),
                in_specs=[smem(), smem()] + [vmem()] * 8,
                out_specs=(vmem(), vmem()) if with_down else (vmem(),),
                cost_estimate=cost,
                compiler_params=pltpu.CompilerParams(vmem_limit_bytes=KERNEL_VMEM),
                name=f"hop_{'first' if hop == 0 else 'both' if with_down else 'up'}",
            )(*operands)
            sent = lax.ppermute(outs[0].astype(jnp.float16), "seq", ahead)
            if with_down:
                down = lax.ppermute(outs[1].astype(jnp.float16), "seq", behind)
                down = down.astype(jnp.float32)
            up = sent.astype(jnp.float32)
    return pl.pallas_call(
        last_kernel,
        out_shape=jax.ShapeDtypeStruct((count, state, width), jnp.float32),
        in_specs=[smem(), smem()] + [vmem()] * 5,
        out_specs=vmem(),
        cost_estimate=cost,
        compiler_params=pltpu.CompilerParams(vmem_limit_bytes=KERNEL_VMEM),
        name="hop_last",
    )(flags(seq_index < half), usable, up, down, *fetched(seq_index))


def swapped(array):
    return lax.ppermute(array, "batch", [(0, 1), (1, 0)])


def local(
    prompt_cache,
    prompt_states,
    block_steps,
    prompt_lengths,
    target_slots,
    cache_lengths,
    resident_cache,
    token_cache,
    queries,
    resident_states,
    decay_rates,
    step_sizes,
    inner_input,
    inner_gate,
    state_input,
    state_readout,
    skip_gain,
):
    seq_count = lax.axis_size("seq")
    seq_index = lax.axis_index("seq")
    batch_index = lax.axis_index("batch")
    local_prompts, block_len, kv_heads, kv_width = prompt_cache.shape
    head_dim = kv_width // 2
    requests = resident_cache.shape[0]
    channels = decay_rates.shape[1]
    local_channels = channels // seq_count

    own_at = batch_index * local_prompts
    peer_at = (1 - batch_index) * local_prompts
    slot_ids = batch_index * requests + jnp.arange(requests, dtype=jnp.int32)
    matches = target_slots[None, :] == slot_ids[:, None]
    fresh = jnp.any(matches, axis=1)
    chosen_len = jnp.sum(jnp.where(matches, prompt_lengths[None, :], 0), axis=1)
    lengths = jnp.where(fresh, chosen_len, cache_lengths)
    own_match = lax.dynamic_slice_in_dim(matches, own_at, local_prompts, 1)
    peer_match = lax.dynamic_slice_in_dim(matches, peer_at, local_prompts, 1)
    own_lengths = lax.dynamic_slice_in_dim(prompt_lengths, own_at, local_prompts)
    usable = (seq_index * block_len < own_lengths).astype(jnp.float32)

    moved = lax.all_to_all(
        jnp.swapaxes(prompt_cache, 0, 1), "seq", split_axis=0, concat_axis=0, tiled=True
    )
    handed = hand_over(
        prompt_states[:, 0], block_steps[:, 0], decay_rates, usable, seq_count, seq_index
    )

    peer_moved = swapped(moved)
    flat = (block_len, local_prompts, kv_heads * kv_width)
    picked = jnp.einsum(
        "rp,ipx->rix",
        own_match.astype(jnp.bfloat16),
        moved.reshape(flat),
        preferred_element_type=jnp.float32,
    ) + jnp.einsum(
        "rp,ipx->rix",
        peer_match.astype(jnp.bfloat16),
        peer_moved.reshape(flat),
        preferred_element_type=jnp.float32,
    )
    picked = picked.astype(jnp.bfloat16).reshape(requests, block_len, kv_heads, kv_width)
    position = jnp.arange(block_len, dtype=jnp.int32) * seq_count + seq_index
    merged = jnp.where(fresh[:, None, None, None], picked, resident_cache[:, :, 0])
    merged = jnp.where(
        (position[None, :] < lengths[:, None])[:, :, None, None],
        merged,
        jnp.zeros((), jnp.bfloat16),
    )
    merged = jnp.where(
        (position[None, :] == lengths[:, None])[:, :, None, None], token_cache[:, None], merged
    )
    heads = queries.shape[1]
    group = heads // kv_heads
    grouped = queries.reshape(requests, kv_heads, group, head_dim)
    scores = jnp.einsum(
        "rgqd,rtgd->rgqt", grouped, merged[..., :head_dim], preferred_element_type=jnp.float32
    ) * (1.0 / math.sqrt(head_dim))
    seen = (position[None, :] <= lengths[:, None])[:, None, None, :]
    masked = jnp.where(seen, scores, -1e30)
    highest = jnp.max(masked, axis=3)
    weights = jnp.where(seen, jnp.exp(masked - highest[..., None]), 0.0)
    denominator = jnp.sum(weights, axis=3)
    summed = jnp.einsum(
        "rgqt,rtgd->rgqd",
        weights.astype(jnp.bfloat16),
        merged[..., head_dim:],
        preferred_element_type=jnp.float32,
    )
    owned = heads // seq_count
    rows = requests * owned
    sums = summed.reshape(requests, seq_count, owned, head_dim)
    sums = jnp.moveaxis(sums, 1, 0).reshape(seq_count, rows, head_dim)
    extra = jnp.stack([highest, denominator]).reshape(2, requests, seq_count, owned)
    extra = jnp.moveaxis(extra, 2, 0).reshape(seq_count, 2 * rows)
    extra = jnp.pad(extra, ((0, 0), (0, head_dim - 2 * rows)))[:, None]
    parcels = lax.all_to_all(
        jnp.concatenate([sums, extra], axis=1), "seq", split_axis=0, concat_axis=0, tiled=True
    )
    peer_sum = parcels[:, :rows]
    peer_top = parcels[:, rows, :rows]
    peer_total = parcels[:, rows, rows : 2 * rows]
    common_top = jnp.max(peer_top, axis=0)
    factor = jnp.exp(peer_top - common_top[None])
    owner_total = jnp.sum(peer_total * factor, axis=0)
    owner_sum = jnp.sum(peer_sum * factor[..., None], axis=0)
    attention = (owner_sum / owner_total[..., None]).astype(jnp.bfloat16)
    attention = attention.reshape(requests, owned, head_dim)

    rates_here = lax.dynamic_slice_in_dim(
        decay_rates, seq_index * local_channels, local_channels, 1
    )
    peer_handed = swapped(handed)
    chosen_state = jnp.sum(
        jnp.where(own_match[:, :, None, None], handed[None], 0.0), axis=1
    ) + jnp.sum(jnp.where(peer_match[:, :, None, None], peer_handed[None], 0.0), axis=1)
    start = jnp.where(fresh[:, None, None], chosen_state, resident_states)
    inner = inner_input.astype(jnp.float32)
    next_states = (
        jnp.exp(-rates_here[None] * step_sizes[:, None, :]) * start
        + (step_sizes * inner)[:, None, :] * state_input[:, :, None]
    )
    readout = jnp.sum(state_readout[:, :, None] * next_states, axis=1) + skip_gain[None, :] * inner
    mamba_output = (readout * jax.nn.silu(inner_gate.astype(jnp.float32))).astype(jnp.bfloat16)
    return (merged[:, :, None], attention, next_states, mamba_output)


def solution(mesh):
    return jax.shard_map(
        local,
        mesh=mesh,
        in_specs=(
            P(("groups", "batch"), "seq", None, None),
            P(("groups", "batch"), "seq", None, None),
            P(("groups", "batch"), "seq", None),
            P("groups"),
            P("groups"),
            P(("groups", "batch")),
            P(("groups", "batch"), None, "seq", None, None),
            P(("groups", "batch"), None, None),
            P(("groups", "batch"), None, None),
            P(("groups", "batch"), None, "seq"),
            P(),
            P(("groups", "batch"), "seq"),
            P(("groups", "batch"), "seq"),
            P(("groups", "batch"), "seq"),
            P(("groups", "batch"), None),
            P(("groups", "batch"), None),
            P("seq"),
        ),
        out_specs=(
            P(("groups", "batch"), None, "seq", None, None),
            P(("groups", "batch"), "seq", None),
            P(("groups", "batch"), None, "seq"),
            P(("groups", "batch"), "seq"),
        ),
        check_vma=False,
    )
```

```python
import functools
import math

import jax
import jax.numpy as jnp
from jax import lax
from jax.experimental import pallas as pl
from jax.experimental.pallas import tpu as pltpu
from jax.sharding import PartitionSpec as P


STATE_SCALE = 128.0
HALF_SPLIT = 8193.0
KERNEL_VMEM = 8 * 1024 * 1024
PAIRS_A_STEP = 4


def split_half(value):
    spread = value * HALF_SPLIT
    high = spread - (spread - value)
    return high, value - high


def smem():
    return pl.BlockSpec(memory_space=pltpu.SMEM)


def vmem():
    return pl.BlockSpec(memory_space=pltpu.VMEM)


def pick_kernel(flags, usable, state_in, step_in, state_out, step_out, *, width):
    count = state_in.shape[0]
    for q in range(PAIRS_A_STEP):
        source = pl.ds(pl.multiple_of(2 * q * width + flags[0] * width, 128), width)
        target = pl.ds(q * width, width)
        for p in range(count):
            use = usable[p]
            state_out[p, :, target] = state_in[p, :, source] * (use * STATE_SCALE)
            step_out[p : p + 1, target] = step_in[p : p + 1, source] * use


def fold_kernel(
    flags, usable, state_in, step_in, rate_in, came_state, came_step, state_out, step_out, rate_out,
    *, width,
):
    count = state_in.shape[0]
    older = flags[1] == 1
    for q in range(PAIRS_A_STEP):
        source = pl.ds(pl.multiple_of(2 * q * width + flags[0] * width, 128), width)
        target = pl.ds(q * width, width)
        rate = rate_in[:, source]
        rate_out[:, target] = rate
        for p in range(count):
            use = usable[p]
            own = state_in[p, :, source] * (use * STATE_SCALE)
            step = step_in[p : p + 1, source] * use
            came, came_by = came_state[p, :, target], came_step[p : p + 1, target]
            early, late = jnp.where(older, own, came), jnp.where(older, came, own)
            late_by = jnp.where(older, came_by, step)
            state_out[p, :, target] = jnp.exp(-rate * late_by) * early + late
            step_out[p : p + 1, target] = step + came_by


def hop_kernel(
    flags, states, steps, rates, up_in, down_in, up_out, down_out=None, *, width, initial
):
    count, state = states.shape[0], states.shape[1]
    rows = count * state
    up_at = pl.ds(pl.multiple_of(flags[0] * width, 128), width)
    down_at = pl.ds(pl.multiple_of(flags[1] * width, 128), width)
    first, last = flags[2] == 1, flags[3] == 1
    up_wrapped, down_wrapped = flags[4] == 1, flags[5] == 1
    up_rate, down_rate = rates[:, up_at], rates[:, down_at]

    @pl.loop(0, count)
    def _(p):
        here = pl.ds(pl.multiple_of(p * state, state), state)
        there = pl.ds(pl.multiple_of(rows + p * state, state), state)
        wide, narrow = pl.ds(2 * rows + p, 1), pl.ds(2 * rows + count + p, 1)
        own, step = states[p, :, up_at], steps[pl.ds(p, 1), up_at]
        if initial:
            acc, aside, span = own, jnp.zeros_like(own), step
        else:
            high, other = up_in[here, :], up_in[there, :]
            whole = high + other
            acc = jnp.where(first, 0.0, jnp.where(up_wrapped, high, whole))
            acc = jnp.exp(-up_rate * step) * acc + own
            aside = jnp.where(first, whole, other)
            span = up_in[wide, :] + up_in[narrow, :]
            span = jnp.where(up_wrapped, span, span + step)
        high, low = split_half(acc)
        up_out[here, :] = high
        up_out[there, :] = low if initial else jnp.where(up_wrapped, aside, low)
        up_out[wide, :], up_out[narrow, :] = split_half(span)
        if down_out is None:
            return
        own, step = states[p, :, down_at], steps[pl.ds(p, 1), down_at]
        if initial:
            acc, aside, span = own, jnp.zeros_like(own), step
        else:
            high, other = down_in[here, :], down_in[there, :]
            whole = high + other
            span = jnp.where(last, 0.0, down_in[wide, :] + down_in[narrow, :])
            acc = jnp.where(last, 0.0, jnp.where(down_wrapped, high, whole))
            acc = acc + jnp.exp(-down_rate * span) * own
            aside = jnp.where(last, whole, other)
            span = span + step
        high, low = split_half(acc)
        down_out[here, :] = high
        down_out[there, :] = low if initial else jnp.where(down_wrapped, aside, low)
        down_out[wide, :], down_out[narrow, :] = split_half(span)


def last_kernel(flags, states, steps, rates, up_in, down_in, handed, *, width):
    count, state = states.shape[0], states.shape[1]
    rows = count * state
    at = pl.ds(pl.multiple_of(flags[0] * width, 128), width)
    first, last = flags[2] == 1, flags[3] == 1
    up_wrapped, down_wrapped = flags[4] == 1, flags[5] == 1
    rate = rates[:, at]

    @pl.loop(0, count)
    def _(p):
        here = pl.ds(pl.multiple_of(p * state, state), state)
        there = pl.ds(pl.multiple_of(rows + p * state, state), state)
        wide, narrow = pl.ds(2 * rows + p, 1), pl.ds(2 * rows + count + p, 1)
        own, step = states[p, :, at], steps[pl.ds(p, 1), at]
        high, other = up_in[here, :], up_in[there, :]
        whole = high + other
        newest = jnp.where(first, whole, jnp.where(up_wrapped, other, 0.0))
        earlier = jnp.where(first, 0.0, jnp.where(up_wrapped, high, whole))
        span = up_in[wide, :] + up_in[narrow, :]
        high, other = down_in[here, :], down_in[there, :]
        whole = high + other
        oldest = jnp.where(last, whole, jnp.where(down_wrapped, other, 0.0))
        later = jnp.where(last, 0.0, jnp.where(down_wrapped, high, whole))
        span_down = jnp.where(last, 0.0, down_in[wide, :] + down_in[narrow, :])
        outer = jnp.where(up_wrapped, span, 0.0)
        inner = earlier + jnp.exp(-rate * span) * oldest
        inner = later + jnp.exp(-rate * span_down) * (own + jnp.exp(-rate * step) * inner)
        handed[p] = (newest + jnp.exp(-rate * outer) * inner) * (1.0 / STATE_SCALE)


def numbers(*values):
    return jnp.stack([jnp.asarray(v) for v in values]).astype(jnp.int32)


def picked_for_pair(states, steps, usable, seq_index, width):
    count, state, channels = states.shape
    wide = PAIRS_A_STEP * width
    return pl.pallas_call(
        functools.partial(pick_kernel, width=width),
        grid=(channels // (2 * wide),),
        out_shape=(
            jax.ShapeDtypeStruct((count, state, channels // 2), jnp.float32),
            jax.ShapeDtypeStruct((count, channels // 2), jnp.float32),
        ),
        in_specs=[
            smem(),
            smem(),
            pl.BlockSpec((count, state, 2 * wide), lambda n: (0, 0, n)),
            pl.BlockSpec((count, 2 * wide), lambda n: (0, n)),
        ],
        out_specs=(
            pl.BlockSpec((count, state, wide), lambda n: (0, 0, n)),
            pl.BlockSpec((count, wide), lambda n: (0, n)),
        ),
        cost_estimate=pl.CostEstimate(
            flops=states.size, bytes_accessed=6 * states.size, transcendentals=0
        ),
        compiler_params=pltpu.CompilerParams(vmem_limit_bytes=2 * KERNEL_VMEM),
        name="pick_for_pair",
    )(numbers(1 - seq_index % 2), usable, states, steps)


def folded_pair(states, steps, rates, usable, came_state, came_step, seq_index, width):
    count, state, channels = states.shape
    wide = PAIRS_A_STEP * width
    parity = seq_index % 2
    return pl.pallas_call(
        functools.partial(fold_kernel, width=width),
        grid=(channels // (2 * wide),),
        out_shape=(
            jax.ShapeDtypeStruct((count, state, channels // 2), jnp.float32),
            jax.ShapeDtypeStruct((count, channels // 2), jnp.float32),
            jax.ShapeDtypeStruct((state, channels // 2), jnp.float32),
        ),
        in_specs=[
            smem(),
            smem(),
            pl.BlockSpec((count, state, 2 * wide), lambda n: (0, 0, n)),
            pl.BlockSpec((count, 2 * wide), lambda n: (0, n)),
            pl.BlockSpec((state, 2 * wide), lambda n: (0, n)),
            pl.BlockSpec((count, state, wide), lambda n: (0, 0, n)),
            pl.BlockSpec((count, wide), lambda n: (0, n)),
        ],
        out_specs=(
            pl.BlockSpec((count, state, wide), lambda n: (0, 0, n)),
            pl.BlockSpec((count, wide), lambda n: (0, n)),
            pl.BlockSpec((state, wide), lambda n: (0, n)),
        ),
        cost_estimate=pl.CostEstimate(
            flops=4 * states.size, bytes_accessed=10 * states.size, transcendentals=states.size
        ),
        compiler_params=pltpu.CompilerParams(vmem_limit_bytes=2 * KERNEL_VMEM),
        name="fold_pair",
    )(numbers(parity, parity == 0), usable, states, steps, rates, came_state, came_step)


def hand_over(states, steps, rates, width, nodes, node):
    count, state, _ = states.shape
    half = nodes // 2
    ring = 2 * nodes
    ahead = [(k, (k + 2) % ring) for k in range(ring)]
    behind = [(k, (k - 2) % ring) for k in range(ring)]
    rows = 2 * count * state + 2 * count
    payload = jax.ShapeDtypeStruct((rows, width), jnp.float32)
    cost = pl.CostEstimate(
        flops=16 * rows * width, bytes_accessed=16 * rows * width, transcendentals=rows * width
    )
    first, last = node == 0, node == nodes - 1
    up = down = jnp.zeros((8, 128), jnp.float32)
    for hop in range(half):
        both = hop < half - 1
        outs = pl.pallas_call(
            functools.partial(hop_kernel, width=width, initial=hop == 0),
            out_shape=(payload, payload) if both else (payload,),
            in_specs=[smem()] + [vmem()] * 5,
            out_specs=(vmem(), vmem()) if both else (vmem(),),
            cost_estimate=cost,
            compiler_params=pltpu.CompilerParams(vmem_limit_bytes=KERNEL_VMEM),
            name="hop_first" if hop == 0 else "hop_both" if both else "hop_up",
        )(
            numbers(
                (node + half - hop) % nodes,
                (node - (half - 1) + hop) % nodes,
                first,
                last,
                node < hop,
                node + hop >= nodes,
            ),
            states,
            steps,
            rates,
            up,
            down,
        )
        sent = lax.ppermute(outs[0].astype(jnp.float16), "seq", ahead)
        if both:
            down = lax.ppermute(outs[1].astype(jnp.float16), "seq", behind)
            down = down.astype(jnp.float32)
        up = sent.astype(jnp.float32)
    return pl.pallas_call(
        functools.partial(last_kernel, width=width),
        out_shape=jax.ShapeDtypeStruct((count, state, width), jnp.float32),
        in_specs=[smem()] + [vmem()] * 5,
        out_specs=vmem(),
        cost_estimate=cost,
        compiler_params=pltpu.CompilerParams(vmem_limit_bytes=KERNEL_VMEM),
        name="hop_last",
    )(
        numbers(node, node, first, last, node < half, node + half - 1 >= nodes),
        states,
        steps,
        rates,
        up,
        down,
    )


def in_pieces(value):
    pieces = []
    for _ in range(3):
        piece = lax.reduce_precision(value, 5, 10)
        pieces.append(piece)
        value = value - piece
    return jnp.stack(pieces)


def swapped(array):
    return lax.ppermute(array, "batch", [(0, 1), (1, 0)])


def local(
    prompt_cache,
    prompt_states,
    block_steps,
    prompt_lengths,
    target_slots,
    cache_lengths,
    resident_cache,
    token_cache,
    queries,
    resident_states,
    decay_rates,
    step_sizes,
    inner_input,
    inner_gate,
    state_input,
    state_readout,
    skip_gain,
):
    seq_count = lax.axis_size("seq")
    seq_index = lax.axis_index("seq")
    batch_index = lax.axis_index("batch")
    local_prompts, block_len, kv_heads, kv_width = prompt_cache.shape
    head_dim = kv_width // 2
    requests = resident_cache.shape[0]
    channels = decay_rates.shape[1]
    local_channels = channels // seq_count

    own_at = batch_index * local_prompts
    peer_at = (1 - batch_index) * local_prompts
    slot_ids = batch_index * requests + jnp.arange(requests, dtype=jnp.int32)
    matches = target_slots[None, :] == slot_ids[:, None]
    fresh = jnp.any(matches, axis=1)
    chosen_len = jnp.sum(jnp.where(matches, prompt_lengths[None, :], 0), axis=1)
    lengths = jnp.where(fresh, chosen_len, cache_lengths)
    own_match = lax.dynamic_slice_in_dim(matches, own_at, local_prompts, 1)
    peer_match = lax.dynamic_slice_in_dim(matches, peer_at, local_prompts, 1)
    own_lengths = lax.dynamic_slice_in_dim(prompt_lengths, own_at, local_prompts)
    usable = (seq_index * block_len < own_lengths).astype(jnp.float32)

    states, steps = prompt_states[:, 0], block_steps[:, 0]
    pairs = [(k, k ^ 1) for k in range(seq_count)]
    sent_state, sent_step = picked_for_pair(states, steps, usable, seq_index, local_channels)
    came_state = lax.ppermute(sent_state.astype(jnp.float16), "seq", pairs)
    came_step = lax.ppermute(sent_step, "seq", pairs)
    moved = lax.all_to_all(
        jnp.swapaxes(prompt_cache, 0, 1), "seq", split_axis=0, concat_axis=0, tiled=True
    )
    folded = folded_pair(
        states,
        steps,
        decay_rates,
        usable,
        came_state.astype(jnp.float32),
        came_step,
        seq_index,
        local_channels,
    )
    handed = hand_over(*folded, local_channels, seq_count // 2, seq_index // 2)

    peer_moved = swapped(moved)
    flat = (block_len, local_prompts, kv_heads * kv_width)
    picked = jnp.einsum(
        "rp,ipx->rix",
        own_match.astype(jnp.bfloat16),
        moved.reshape(flat),
        preferred_element_type=jnp.float32,
    ) + jnp.einsum(
        "rp,ipx->rix",
        peer_match.astype(jnp.bfloat16),
        peer_moved.reshape(flat),
        preferred_element_type=jnp.float32,
    )
    picked = picked.astype(jnp.bfloat16).reshape(requests, block_len, kv_heads, kv_width)
    position = jnp.arange(block_len, dtype=jnp.int32) * seq_count + seq_index
    merged = jnp.where(fresh[:, None, None, None], picked, resident_cache[:, :, 0])
    merged = jnp.where(
        (position[None, :] < lengths[:, None])[:, :, None, None],
        merged,
        jnp.zeros((), jnp.bfloat16),
    )
    merged = jnp.where(
        (position[None, :] == lengths[:, None])[:, :, None, None], token_cache[:, None], merged
    )
    heads = queries.shape[1]
    group = heads // kv_heads
    grouped = queries.reshape(requests, kv_heads, group, head_dim)
    scores = jnp.einsum(
        "rgqd,rtgd->rgqt", grouped, merged[..., :head_dim], preferred_element_type=jnp.float32
    ) * (1.0 / math.sqrt(head_dim))
    seen = (position[None, :] <= lengths[:, None])[:, None, None, :]
    masked = jnp.where(seen, scores, -1e30)
    highest = jnp.max(masked, axis=3)
    weights = jnp.where(seen, jnp.exp(masked - highest[..., None]), 0.0)
    denominator = jnp.sum(weights, axis=3)
    summed = jnp.einsum(
        "rgqt,rtgd->rgqd",
        weights.astype(jnp.bfloat16),
        merged[..., head_dim:],
        preferred_element_type=jnp.float32,
    )
    owned = heads // seq_count
    rows = requests * owned
    sums = summed.reshape(requests, seq_count, owned, head_dim)
    sums = jnp.moveaxis(sums, 1, 0).reshape(seq_count, rows, head_dim)
    extra = in_pieces(jnp.stack([highest, denominator])).reshape(6, requests, seq_count, owned)
    extra = jnp.moveaxis(extra, 2, 0).reshape(seq_count, 6 * rows)
    extra = jnp.pad(extra, ((0, 0), (0, head_dim - 6 * rows)))[:, None]
    parcels = lax.all_to_all(
        jnp.concatenate([sums, extra], axis=1).astype(jnp.float16),
        "seq",
        split_axis=0,
        concat_axis=0,
        tiled=True,
    ).astype(jnp.float32)
    peer_sum = parcels[:, :rows]
    peer_extra = parcels[:, rows, : 6 * rows].reshape(seq_count, 3, 2, rows)
    peer_extra = (peer_extra[:, 2] + peer_extra[:, 1]) + peer_extra[:, 0]
    peer_top, peer_total = peer_extra[:, 0], peer_extra[:, 1]
    common_top = jnp.max(peer_top, axis=0)
    factor = jnp.exp(peer_top - common_top[None])
    owner_total = jnp.sum(peer_total * factor, axis=0)
    owner_sum = jnp.sum(peer_sum * factor[..., None], axis=0)
    attention = (owner_sum / owner_total[..., None]).astype(jnp.bfloat16)
    attention = attention.reshape(requests, owned, head_dim)

    rates_here = lax.dynamic_slice_in_dim(
        decay_rates, seq_index * local_channels, local_channels, 1
    )
    peer_handed = swapped(handed)
    chosen_state = jnp.sum(
        jnp.where(own_match[:, :, None, None], handed[None], 0.0), axis=1
    ) + jnp.sum(jnp.where(peer_match[:, :, None, None], peer_handed[None], 0.0), axis=1)
    start = jnp.where(fresh[:, None, None], chosen_state, resident_states)
    inner = inner_input.astype(jnp.float32)
    next_states = (
        jnp.exp(-rates_here[None] * step_sizes[:, None, :]) * start
        + (step_sizes * inner)[:, None, :] * state_input[:, :, None]
    )
    readout = jnp.sum(state_readout[:, :, None] * next_states, axis=1) + skip_gain[None, :] * inner
    mamba_output = (readout * jax.nn.silu(inner_gate.astype(jnp.float32))).astype(jnp.bfloat16)
    return (merged[:, :, None], attention, next_states, mamba_output)


def solution(mesh):
    return jax.shard_map(
        local,
        mesh=mesh,
        in_specs=(
            P(("groups", "batch"), "seq", None, None),
            P(("groups", "batch"), "seq", None, None),
            P(("groups", "batch"), "seq", None),
            P("groups"),
            P("groups"),
            P(("groups", "batch")),
            P(("groups", "batch"), None, "seq", None, None),
            P(("groups", "batch"), None, None),
            P(("groups", "batch"), None, None),
            P(("groups", "batch"), None, "seq"),
            P(),
            P(("groups", "batch"), "seq"),
            P(("groups", "batch"), "seq"),
            P(("groups", "batch"), "seq"),
            P(("groups", "batch"), None),
            P(("groups", "batch"), None),
            P("seq"),
        ),
        out_specs=(
            P(("groups", "batch"), None, "seq", None, None),
            P(("groups", "batch"), "seq", None),
            P(("groups", "batch"), None, "seq"),
            P(("groups", "batch"), "seq"),
        ),
        check_vma=False,
    )
```

```python
import functools
import math

import jax
import jax.numpy as jnp
from jax import lax
from jax.experimental import pallas as pl
from jax.experimental.pallas import tpu as pltpu
from jax.sharding import PartitionSpec as P


STATE_SCALE = 128.0
HALF_SPLIT = 8193.0
KERNEL_VMEM = 8 * 1024 * 1024
PAIRS_A_STEP = 4


def split_half(value):
    spread = value * HALF_SPLIT
    high = spread - (spread - value)
    return high, value - high


def smem():
    return pl.BlockSpec(memory_space=pltpu.SMEM)


def vmem():
    return pl.BlockSpec(memory_space=pltpu.VMEM)


def pick_kernel(
    flags, usable, state_in, step_in, rate_in, sent_state, sent_step, own_state, own_step, own_rate,
    *, width,
):
    count = state_in.shape[0]
    for q in range(PAIRS_A_STEP):
        own = pl.ds(pl.multiple_of((2 * q + flags[0]) * width, 128), width)
        other = pl.ds(pl.multiple_of((2 * q + flags[1]) * width, 128), width)
        target = pl.ds(q * width, width)
        own_rate[:, target] = rate_in[:, own]
        for p in range(count):
            use = usable[p]
            sent_state[p, :, target] = state_in[p, :, other] * (use * STATE_SCALE)
            own_state[p, :, target] = state_in[p, :, own] * (use * STATE_SCALE)
            sent_step[p : p + 1, target] = step_in[p, :, other] * use
            own_step[p : p + 1, target] = step_in[p, :, own] * use


def fold_kernel(
    flags, own_state, own_step, rates, came_state, came_step, state_out, step_out, *, width
):
    count = own_state.shape[0]
    older = flags[0] == 0

    @pl.loop(0, own_state.shape[2] // width)
    def _(q):
        at = pl.ds(pl.multiple_of(q * width, 128), width)
        rate = rates[:, at]
        for p in range(count):
            own, came = own_state[p, :, at], came_state[p, :, at]
            step, came_by = own_step[p : p + 1, at], came_step[p : p + 1, at]
            early, late = jnp.where(older, own, came), jnp.where(older, came, own)
            late_by = jnp.where(older, came_by, step)
            state_out[p, :, at] = jnp.exp(-rate * late_by) * early + late
            step_out[p : p + 1, at] = step + came_by


def hop_kernel(
    flags, states, steps, rates, up_in, down_in, up_out, down_out=None, *, width, initial
):
    count, state = states.shape[0], states.shape[1]
    rows = count * state
    up_at = pl.ds(pl.multiple_of(flags[0] * width, 128), width)
    down_at = pl.ds(pl.multiple_of(flags[1] * width, 128), width)
    first, last = flags[2] == 1, flags[3] == 1
    up_wrapped, down_wrapped = flags[4] == 1, flags[5] == 1
    up_rate, down_rate = rates[:, up_at], rates[:, down_at]

    @pl.loop(0, count, unroll=True)
    def _(p):
        here = pl.ds(pl.multiple_of(p * state, state), state)
        there = pl.ds(pl.multiple_of(rows + p * state, state), state)
        wide, narrow = pl.ds(2 * rows + p, 1), pl.ds(2 * rows + count + p, 1)
        own, step = states[p, :, up_at], steps[pl.ds(p, 1), up_at]
        if initial:
            acc, aside, span = own, jnp.zeros_like(own), step
        else:
            high, other = up_in[here, :], up_in[there, :]
            whole = high + other
            acc = jnp.where(first, 0.0, jnp.where(up_wrapped, high, whole))
            acc = jnp.exp(-up_rate * step) * acc + own
            aside = jnp.where(first, whole, other)
            span = up_in[wide, :] + up_in[narrow, :]
            span = jnp.where(up_wrapped, span, span + step)
        high, low = split_half(acc)
        up_out[here, :] = high
        up_out[there, :] = low if initial else jnp.where(up_wrapped, aside, low)
        up_out[wide, :], up_out[narrow, :] = split_half(span)
        if down_out is None:
            return
        own, step = states[p, :, down_at], steps[pl.ds(p, 1), down_at]
        if initial:
            acc, aside, span = own, jnp.zeros_like(own), step
        else:
            high, other = down_in[here, :], down_in[there, :]
            whole = high + other
            span = jnp.where(last, 0.0, down_in[wide, :] + down_in[narrow, :])
            acc = jnp.where(last, 0.0, jnp.where(down_wrapped, high, whole))
            acc = acc + jnp.exp(-down_rate * span) * own
            aside = jnp.where(last, whole, other)
            span = span + step
        high, low = split_half(acc)
        down_out[here, :] = high
        down_out[there, :] = low if initial else jnp.where(down_wrapped, aside, low)
        down_out[wide, :], down_out[narrow, :] = split_half(span)


def last_kernel(flags, states, steps, rates, up_in, down_in, handed, *, width):
    count, state = states.shape[0], states.shape[1]
    rows = count * state
    at = pl.ds(pl.multiple_of(flags[0] * width, 128), width)
    first, last = flags[2] == 1, flags[3] == 1
    up_wrapped, down_wrapped = flags[4] == 1, flags[5] == 1
    rate = rates[:, at]

    @pl.loop(0, count, unroll=True)
    def _(p):
        here = pl.ds(pl.multiple_of(p * state, state), state)
        there = pl.ds(pl.multiple_of(rows + p * state, state), state)
        wide, narrow = pl.ds(2 * rows + p, 1), pl.ds(2 * rows + count + p, 1)
        own, step = states[p, :, at], steps[pl.ds(p, 1), at]
        high, other = up_in[here, :], up_in[there, :]
        whole = high + other
        newest = jnp.where(first, whole, jnp.where(up_wrapped, other, 0.0))
        earlier = jnp.where(first, 0.0, jnp.where(up_wrapped, high, whole))
        span = up_in[wide, :] + up_in[narrow, :]
        high, other = down_in[here, :], down_in[there, :]
        whole = high + other
        oldest = jnp.where(last, whole, jnp.where(down_wrapped, other, 0.0))
        later = jnp.where(last, 0.0, jnp.where(down_wrapped, high, whole))
        span_down = jnp.where(last, 0.0, down_in[wide, :] + down_in[narrow, :])
        outer = jnp.where(up_wrapped, span, 0.0)
        inner = earlier + jnp.exp(-rate * span) * oldest
        inner = later + jnp.exp(-rate * span_down) * (own + jnp.exp(-rate * step) * inner)
        handed[p] = (newest + jnp.exp(-rate * outer) * inner) * (1.0 / STATE_SCALE)


def numbers(*values):
    return jnp.stack([jnp.asarray(v) for v in values]).astype(jnp.int32)


def picked_for_pair(states, steps, rates, usable, seq_index, width):
    count, state, channels = states.shape
    wide = PAIRS_A_STEP * width
    blocks = (
        pl.BlockSpec((count, state, wide), lambda n: (0, 0, n)),
        pl.BlockSpec((count, wide), lambda n: (0, n)),
    )
    shapes = (
        jax.ShapeDtypeStruct((count, state, channels // 2), jnp.float32),
        jax.ShapeDtypeStruct((count, channels // 2), jnp.float32),
    )
    return pl.pallas_call(
        functools.partial(pick_kernel, width=width),
        grid=(channels // (2 * wide),),
        out_shape=shapes
        + shapes
        + (jax.ShapeDtypeStruct((state, channels // 2), jnp.float32),),
        in_specs=[
            smem(),
            smem(),
            pl.BlockSpec((count, state, 2 * wide), lambda n: (0, 0, n)),
            pl.BlockSpec((count, 1, 2 * wide), lambda n: (0, 0, n)),
            pl.BlockSpec((state, 2 * wide), lambda n: (0, n)),
        ],
        out_specs=blocks + blocks + (pl.BlockSpec((state, wide), lambda n: (0, n)),),
        cost_estimate=pl.CostEstimate(
            flops=states.size, bytes_accessed=8 * states.size, transcendentals=0
        ),
        compiler_params=pltpu.CompilerParams(vmem_limit_bytes=7 * KERNEL_VMEM),
        name="pick_for_pair",
    )(numbers(seq_index % 2, 1 - seq_index % 2), usable, states, steps, rates)


def folded_pair(own_state, own_step, rates, came_state, came_step, seq_index, width):
    return pl.pallas_call(
        functools.partial(fold_kernel, width=width),
        out_shape=(
            jax.ShapeDtypeStruct(own_state.shape, jnp.float32),
            jax.ShapeDtypeStruct(own_step.shape, jnp.float32),
        ),
        in_specs=[smem()] + [vmem()] * 5,
        out_specs=(vmem(), vmem()),
        cost_estimate=pl.CostEstimate(
            flops=4 * own_state.size,
            bytes_accessed=12 * own_state.size,
            transcendentals=own_state.size,
        ),
        compiler_params=pltpu.CompilerParams(vmem_limit_bytes=KERNEL_VMEM),
        name="fold_pair",
    )(numbers(seq_index % 2), own_state, own_step, rates, came_state, came_step)


def hand_over(states, steps, rates, width, nodes, node):
    count, state, _ = states.shape
    half = nodes // 2
    ring = 2 * nodes
    ahead = [(k, (k + 2) % ring) for k in range(ring)]
    behind = [(k, (k - 2) % ring) for k in range(ring)]
    rows = 2 * count * state + 2 * count
    payload = jax.ShapeDtypeStruct((rows, width), jnp.float32)
    cost = pl.CostEstimate(
        flops=16 * rows * width, bytes_accessed=16 * rows * width, transcendentals=rows * width
    )
    first, last = node == 0, node == nodes - 1
    up = down = jnp.zeros((8, 128), jnp.float32)
    for hop in range(half):
        both = hop < half - 1
        outs = pl.pallas_call(
            functools.partial(hop_kernel, width=width, initial=hop == 0),
            out_shape=(payload, payload) if both else (payload,),
            in_specs=[smem()] + [vmem()] * 5,
            out_specs=(vmem(), vmem()) if both else (vmem(),),
            cost_estimate=cost,
            compiler_params=pltpu.CompilerParams(vmem_limit_bytes=KERNEL_VMEM),
            name="hop_first" if hop == 0 else "hop_both" if both else "hop_up",
        )(
            numbers(
                (node + half - hop) % nodes,
                (node - (half - 1) + hop) % nodes,
                first,
                last,
                node < hop,
                node + hop >= nodes,
            ),
            states,
            steps,
            rates,
            up,
            down,
        )
        sent = lax.ppermute(outs[0].astype(jnp.float16), "seq", ahead)
        if both:
            down = lax.ppermute(outs[1].astype(jnp.float16), "seq", behind)
            down = down.astype(jnp.float32)
        up = sent.astype(jnp.float32)
    return pl.pallas_call(
        functools.partial(last_kernel, width=width),
        out_shape=jax.ShapeDtypeStruct((count, state, width), jnp.float32),
        in_specs=[smem()] + [vmem()] * 5,
        out_specs=vmem(),
        cost_estimate=cost,
        compiler_params=pltpu.CompilerParams(vmem_limit_bytes=KERNEL_VMEM),
        name="hop_last",
    )(
        numbers(node, node, first, last, node < half, node + half - 1 >= nodes),
        states,
        steps,
        rates,
        up,
        down,
    )


def in_pieces(value):
    pieces = []
    for _ in range(3):
        piece = lax.reduce_precision(value, 5, 10)
        pieces.append(piece)
        value = value - piece
    return jnp.stack(pieces)


def swapped(array):
    return lax.ppermute(array, "batch", [(0, 1), (1, 0)])


def local(
    prompt_cache,
    prompt_states,
    block_steps,
    prompt_lengths,
    target_slots,
    cache_lengths,
    resident_cache,
    token_cache,
    queries,
    resident_states,
    decay_rates,
    step_sizes,
    inner_input,
    inner_gate,
    state_input,
    state_readout,
    skip_gain,
):
    seq_count = lax.axis_size("seq")
    seq_index = lax.axis_index("seq")
    batch_index = lax.axis_index("batch")
    local_prompts, block_len, kv_heads, kv_width = prompt_cache.shape
    head_dim = kv_width // 2
    requests = resident_cache.shape[0]
    channels = decay_rates.shape[1]
    local_channels = channels // seq_count

    own_at = batch_index * local_prompts
    peer_at = (1 - batch_index) * local_prompts
    slot_ids = batch_index * requests + jnp.arange(requests, dtype=jnp.int32)
    matches = target_slots[None, :] == slot_ids[:, None]
    fresh = jnp.any(matches, axis=1)
    chosen_len = jnp.sum(jnp.where(matches, prompt_lengths[None, :], 0), axis=1)
    lengths = jnp.where(fresh, chosen_len, cache_lengths)
    own_match = lax.dynamic_slice_in_dim(matches, own_at, local_prompts, 1)
    peer_match = lax.dynamic_slice_in_dim(matches, peer_at, local_prompts, 1)
    own_lengths = lax.dynamic_slice_in_dim(prompt_lengths, own_at, local_prompts)
    usable = (seq_index * block_len < own_lengths).astype(jnp.float32)

    pairs = [(k, k ^ 1) for k in range(seq_count)]
    sent_state, sent_step, own_state, own_step, rates = picked_for_pair(
        prompt_states[:, 0], block_steps, decay_rates, usable, seq_index, local_channels
    )
    came_state = lax.ppermute(sent_state.astype(jnp.float16), "seq", pairs)
    came_step = lax.ppermute(sent_step, "seq", pairs)
    moved = lax.all_to_all(
        jnp.swapaxes(prompt_cache, 0, 1), "seq", split_axis=0, concat_axis=0, tiled=True
    )
    folded = folded_pair(
        own_state,
        own_step,
        rates,
        came_state.astype(jnp.float32),
        came_step,
        seq_index,
        local_channels,
    )
    handed = hand_over(*folded, rates, local_channels, seq_count // 2, seq_index // 2)

    peer_moved = swapped(moved)
    flat = (block_len, local_prompts, kv_heads * kv_width)
    picked = jnp.einsum(
        "rp,ipx->rix",
        own_match.astype(jnp.bfloat16),
        moved.reshape(flat),
        preferred_element_type=jnp.float32,
    ) + jnp.einsum(
        "rp,ipx->rix",
        peer_match.astype(jnp.bfloat16),
        peer_moved.reshape(flat),
        preferred_element_type=jnp.float32,
    )
    picked = picked.astype(jnp.bfloat16).reshape(requests, block_len, kv_heads, kv_width)
    position = jnp.arange(block_len, dtype=jnp.int32) * seq_count + seq_index
    merged = jnp.where(fresh[:, None, None, None], picked, resident_cache[:, :, 0])
    merged = jnp.where(
        (position[None, :] < lengths[:, None])[:, :, None, None],
        merged,
        jnp.zeros((), jnp.bfloat16),
    )
    merged = jnp.where(
        (position[None, :] == lengths[:, None])[:, :, None, None], token_cache[:, None], merged
    )
    heads = queries.shape[1]
    group = heads // kv_heads
    grouped = queries.reshape(requests, kv_heads, group, head_dim)
    scores = jnp.einsum(
        "rgqd,rtgd->rgqt", grouped, merged[..., :head_dim], preferred_element_type=jnp.float32
    ) * (1.0 / math.sqrt(head_dim))
    seen = (position[None, :] <= lengths[:, None])[:, None, None, :]
    masked = jnp.where(seen, scores, -1e30)
    highest = jnp.max(masked, axis=3)
    weights = jnp.where(seen, jnp.exp(masked - highest[..., None]), 0.0)
    denominator = jnp.sum(weights, axis=3)
    summed = jnp.einsum(
        "rgqt,rtgd->rgqd",
        weights.astype(jnp.bfloat16),
        merged[..., head_dim:],
        preferred_element_type=jnp.float32,
    )
    owned = heads // seq_count
    rows = requests * owned
    sums = summed.reshape(requests, seq_count, owned, head_dim)
    sums = jnp.moveaxis(sums, 1, 0).reshape(seq_count, rows, head_dim)
    extra = in_pieces(jnp.stack([highest, denominator])).reshape(6, requests, seq_count, owned)
    extra = jnp.moveaxis(extra, 2, 0).reshape(seq_count, 6 * rows)
    extra = jnp.pad(extra, ((0, 0), (0, head_dim - 6 * rows)))[:, None]
    parcels = lax.all_to_all(
        jnp.concatenate([sums, extra], axis=1).astype(jnp.float16),
        "seq",
        split_axis=0,
        concat_axis=0,
        tiled=True,
    ).astype(jnp.float32)
    peer_sum = parcels[:, :rows]
    peer_extra = parcels[:, rows, : 6 * rows].reshape(seq_count, 3, 2, rows)
    peer_extra = (peer_extra[:, 2] + peer_extra[:, 1]) + peer_extra[:, 0]
    peer_top, peer_total = peer_extra[:, 0], peer_extra[:, 1]
    common_top = jnp.max(peer_top, axis=0)
    factor = jnp.exp(peer_top - common_top[None])
    owner_total = jnp.sum(peer_total * factor, axis=0)
    owner_sum = jnp.sum(peer_sum * factor[..., None], axis=0)
    attention = (owner_sum / owner_total[..., None]).astype(jnp.bfloat16)
    attention = attention.reshape(requests, owned, head_dim)

    rates_here = lax.dynamic_slice_in_dim(
        decay_rates, seq_index * local_channels, local_channels, 1
    )
    peer_handed = swapped(handed)
    chosen_state = jnp.sum(
        jnp.where(own_match[:, :, None, None], handed[None], 0.0), axis=1
    ) + jnp.sum(jnp.where(peer_match[:, :, None, None], peer_handed[None], 0.0), axis=1)
    start = jnp.where(fresh[:, None, None], chosen_state, resident_states)
    inner = inner_input.astype(jnp.float32)
    next_states = (
        jnp.exp(-rates_here[None] * step_sizes[:, None, :]) * start
        + (step_sizes * inner)[:, None, :] * state_input[:, :, None]
    )
    readout = jnp.sum(state_readout[:, :, None] * next_states, axis=1) + skip_gain[None, :] * inner
    mamba_output = (readout * jax.nn.silu(inner_gate.astype(jnp.float32))).astype(jnp.bfloat16)
    return (merged[:, :, None], attention, next_states, mamba_output)


def solution(mesh):
    return jax.shard_map(
        local,
        mesh=mesh,
        in_specs=(
            P(("groups", "batch"), "seq", None, None),
            P(("groups", "batch"), "seq", None, None),
            P(("groups", "batch"), "seq", None),
            P("groups"),
            P("groups"),
            P(("groups", "batch")),
            P(("groups", "batch"), None, "seq", None, None),
            P(("groups", "batch"), None, None),
            P(("groups", "batch"), None, None),
            P(("groups", "batch"), None, "seq"),
            P(),
            P(("groups", "batch"), "seq"),
            P(("groups", "batch"), "seq"),
            P(("groups", "batch"), "seq"),
            P(("groups", "batch"), None),
            P(("groups", "batch"), None),
            P("seq"),
        ),
        out_specs=(
            P(("groups", "batch"), None, "seq", None, None),
            P(("groups", "batch"), "seq", None),
            P(("groups", "batch"), None, "seq"),
            P(("groups", "batch"), "seq"),
        ),
        check_vma=False,
    )
```

```python
import functools
import math

import jax
import jax.numpy as jnp
from jax import lax
from jax.experimental import pallas as pl
from jax.experimental.pallas import tpu as pltpu
from jax.sharding import PartitionSpec as P


STATE_SCALE = 128.0
HALF_SPLIT = 8193.0
KERNEL_VMEM = 8 * 1024 * 1024
PAIRS_A_STEP = 4


def split_half(value):
    spread = value * HALF_SPLIT
    high = spread - (spread - value)
    return high, value - high


def smem():
    return pl.BlockSpec(memory_space=pltpu.SMEM)


def vmem():
    return pl.BlockSpec(memory_space=pltpu.VMEM)


def pick_kernel(where, lengths, state_in, step_in, state_out, step_out, *, width):
    count = state_in.shape[0]
    for p in range(count):
        use = jnp.where(where[1] < lengths[where[2] + p], 1.0, 0.0)
        for q in range(PAIRS_A_STEP):
            source = pl.ds(pl.multiple_of((2 * q + where[0]) * width, 128), width)
            target = pl.ds(q * width, width)
            state_out[p, :, target] = state_in[p, :, source] * (use * STATE_SCALE)
            step_out[p : p + 1, target] = step_in[p, :, source] * use


def rate_kernel(where, rate_in, rate_out, *, width):
    for q in range(PAIRS_A_STEP):
        source = pl.ds(pl.multiple_of((2 * q + where[0]) * width, 128), width)
        rate_out[:, q * width : (q + 1) * width] = rate_in[:, source]


def fold_kernel(
    flags, own_state, own_step, rates, came_state, came_step, state_out, step_out, *, width
):
    count = own_state.shape[0]
    older = flags[0] == 0

    @pl.loop(0, own_state.shape[2] // width)
    def _(q):
        at = pl.ds(pl.multiple_of(q * width, 128), width)
        rate = rates[:, at]
        for p in range(count):
            own, came = own_state[p, :, at], came_state[p, :, at]
            step, came_by = own_step[p : p + 1, at], came_step[p : p + 1, at]
            early, late = jnp.where(older, own, came), jnp.where(older, came, own)
            late_by = jnp.where(older, came_by, step)
            state_out[p, :, at] = jnp.exp(-rate * late_by) * early + late
            step_out[p : p + 1, at] = step + came_by


def hop_kernel(
    flags, states, steps, rates, up_in, down_in, up_out, down_out=None, *, width, initial
):
    count, state = states.shape[0], states.shape[1]
    rows = count * state
    up_at = pl.ds(pl.multiple_of(flags[0] * width, 128), width)
    down_at = pl.ds(pl.multiple_of(flags[1] * width, 128), width)
    first, last = flags[2] == 1, flags[3] == 1
    up_wrapped, down_wrapped = flags[4] == 1, flags[5] == 1
    up_rate, down_rate = rates[:, up_at], rates[:, down_at]

    @pl.loop(0, count, unroll=True)
    def _(p):
        here = pl.ds(pl.multiple_of(p * state, state), state)
        there = pl.ds(pl.multiple_of(rows + p * state, state), state)
        wide, narrow = pl.ds(2 * rows + p, 1), pl.ds(2 * rows + count + p, 1)
        own, step = states[p, :, up_at], steps[pl.ds(p, 1), up_at]
        if initial:
            acc, aside, span = own, jnp.zeros_like(own), step
        else:
            high, other = up_in[here, :], up_in[there, :]
            whole = high + other
            acc = jnp.where(first, 0.0, jnp.where(up_wrapped, high, whole))
            acc = jnp.exp(-up_rate * step) * acc + own
            aside = jnp.where(first, whole, other)
            span = up_in[wide, :] + up_in[narrow, :]
            span = jnp.where(up_wrapped, span, span + step)
        high, low = split_half(acc)
        up_out[here, :] = high
        up_out[there, :] = low if initial else jnp.where(up_wrapped, aside, low)
        up_out[wide, :], up_out[narrow, :] = split_half(span)
        if down_out is None:
            return
        own, step = states[p, :, down_at], steps[pl.ds(p, 1), down_at]
        if initial:
            acc, aside, span = own, jnp.zeros_like(own), step
        else:
            high, other = down_in[here, :], down_in[there, :]
            whole = high + other
            span = jnp.where(last, 0.0, down_in[wide, :] + down_in[narrow, :])
            acc = jnp.where(last, 0.0, jnp.where(down_wrapped, high, whole))
            acc = acc + jnp.exp(-down_rate * span) * own
            aside = jnp.where(last, whole, other)
            span = span + step
        high, low = split_half(acc)
        down_out[here, :] = high
        down_out[there, :] = low if initial else jnp.where(down_wrapped, aside, low)
        down_out[wide, :], down_out[narrow, :] = split_half(span)


def last_kernel(flags, states, steps, rates, up_in, down_in, handed, *, width):
    count, state = states.shape[0], states.shape[1]
    rows = count * state
    at = pl.ds(pl.multiple_of(flags[0] * width, 128), width)
    first, last = flags[2] == 1, flags[3] == 1
    up_wrapped, down_wrapped = flags[4] == 1, flags[5] == 1
    rate = rates[:, at]

    @pl.loop(0, count, unroll=True)
    def _(p):
        here = pl.ds(pl.multiple_of(p * state, state), state)
        there = pl.ds(pl.multiple_of(rows + p * state, state), state)
        wide, narrow = pl.ds(2 * rows + p, 1), pl.ds(2 * rows + count + p, 1)
        own, step = states[p, :, at], steps[pl.ds(p, 1), at]
        high, other = up_in[here, :], up_in[there, :]
        whole = high + other
        newest = jnp.where(first, whole, jnp.where(up_wrapped, other, 0.0))
        earlier = jnp.where(first, 0.0, jnp.where(up_wrapped, high, whole))
        span = up_in[wide, :] + up_in[narrow, :]
        high, other = down_in[here, :], down_in[there, :]
        whole = high + other
        oldest = jnp.where(last, whole, jnp.where(down_wrapped, other, 0.0))
        later = jnp.where(last, 0.0, jnp.where(down_wrapped, high, whole))
        span_down = jnp.where(last, 0.0, down_in[wide, :] + down_in[narrow, :])
        outer = jnp.where(up_wrapped, span, 0.0)
        inner = earlier + jnp.exp(-rate * span) * oldest
        inner = later + jnp.exp(-rate * span_down) * (own + jnp.exp(-rate * step) * inner)
        handed[p] = (newest + jnp.exp(-rate * outer) * inner) * (1.0 / STATE_SCALE)


def numbers(*values):
    return jnp.stack([jnp.asarray(v) for v in values]).astype(jnp.int32)


def pick(where, lengths, states, steps, width):
    count, state, channels = states.shape
    wide = PAIRS_A_STEP * width
    return pl.pallas_call(
        functools.partial(pick_kernel, width=width),
        grid=(channels // (2 * wide),),
        out_shape=(
            jax.ShapeDtypeStruct((count, state, channels // 2), jnp.float32),
            jax.ShapeDtypeStruct((count, channels // 2), jnp.float32),
        ),
        in_specs=[
            smem(),
            smem(),
            pl.BlockSpec((count, state, 2 * wide), lambda n: (0, 0, n)),
            pl.BlockSpec((count, 1, 2 * wide), lambda n: (0, 0, n)),
        ],
        out_specs=(
            pl.BlockSpec((count, state, wide), lambda n: (0, 0, n)),
            pl.BlockSpec((count, wide), lambda n: (0, n)),
        ),
        cost_estimate=pl.CostEstimate(
            flops=states.size, bytes_accessed=6 * states.size, transcendentals=0
        ),
        compiler_params=pltpu.CompilerParams(vmem_limit_bytes=56 * 1024 * 1024),
    )(where, lengths, states, steps)


def picked_rates(where, rates, width):
    state, channels = rates.shape
    wide = PAIRS_A_STEP * width
    return pl.pallas_call(
        functools.partial(rate_kernel, width=width),
        grid=(channels // (2 * wide),),
        out_shape=jax.ShapeDtypeStruct((state, channels // 2), jnp.float32),
        in_specs=[smem(), pl.BlockSpec((state, 2 * wide), lambda n: (0, n))],
        out_specs=pl.BlockSpec((state, wide), lambda n: (0, n)),
        cost_estimate=pl.CostEstimate(
            flops=0, bytes_accessed=6 * rates.size, transcendentals=0
        ),
        compiler_params=pltpu.CompilerParams(vmem_limit_bytes=56 * 1024 * 1024),
        name="pick_rates",
    )(where, rates)


def folded_pair(own_state, own_step, rates, came_state, came_step, seq_index, width):
    return pl.pallas_call(
        functools.partial(fold_kernel, width=width),
        out_shape=(
            jax.ShapeDtypeStruct(own_state.shape, jnp.float32),
            jax.ShapeDtypeStruct(own_step.shape, jnp.float32),
        ),
        in_specs=[smem()] + [vmem()] * 5,
        out_specs=(vmem(), vmem()),
        cost_estimate=pl.CostEstimate(
            flops=4 * own_state.size,
            bytes_accessed=12 * own_state.size,
            transcendentals=own_state.size,
        ),
        compiler_params=pltpu.CompilerParams(vmem_limit_bytes=KERNEL_VMEM),
        name="fold_pair",
    )(numbers(seq_index % 2), own_state, own_step, rates, came_state, came_step)


def hand_over(states, steps, rates, width, nodes, node):
    count, state, _ = states.shape
    half = nodes // 2
    ring = 2 * nodes
    ahead = [(k, (k + 2) % ring) for k in range(ring)]
    behind = [(k, (k - 2) % ring) for k in range(ring)]
    rows = 2 * count * state + 2 * count
    payload = jax.ShapeDtypeStruct((rows, width), jnp.float32)
    cost = pl.CostEstimate(
        flops=16 * rows * width, bytes_accessed=16 * rows * width, transcendentals=rows * width
    )
    first, last = node == 0, node == nodes - 1
    up = down = jnp.zeros((8, 128), jnp.float32)
    for hop in range(half):
        both = hop < half - 1
        outs = pl.pallas_call(
            functools.partial(hop_kernel, width=width, initial=hop == 0),
            out_shape=(payload, payload) if both else (payload,),
            in_specs=[smem()] + [vmem()] * 5,
            out_specs=(vmem(), vmem()) if both else (vmem(),),
            cost_estimate=cost,
            compiler_params=pltpu.CompilerParams(vmem_limit_bytes=KERNEL_VMEM),
            name="hop_first" if hop == 0 else "hop_both" if both else "hop_up",
        )(
            numbers(
                (node + half - hop) % nodes,
                (node - (half - 1) + hop) % nodes,
                first,
                last,
                node < hop,
                node + hop >= nodes,
            ),
            states,
            steps,
            rates,
            up,
            down,
        )
        sent = lax.ppermute(outs[0].astype(jnp.float16), "seq", ahead)
        if both:
            down = lax.ppermute(outs[1].astype(jnp.float16), "seq", behind)
            down = down.astype(jnp.float32)
        up = sent.astype(jnp.float32)
    return pl.pallas_call(
        functools.partial(last_kernel, width=width),
        out_shape=jax.ShapeDtypeStruct((count, state, width), jnp.float32),
        in_specs=[smem()] + [vmem()] * 5,
        out_specs=vmem(),
        cost_estimate=cost,
        compiler_params=pltpu.CompilerParams(vmem_limit_bytes=KERNEL_VMEM),
        name="hop_last",
    )(
        numbers(node, node, first, last, node < half, node + half - 1 >= nodes),
        states,
        steps,
        rates,
        up,
        down,
    )


def owners_first(value, seq_count, owned, *minor):
    bits = seq_count.bit_length() - 1
    requests = value.shape[0]
    value = value.reshape(requests, *(2,) * bits, owned, *minor)
    value = value.transpose(*range(bits, 0, -1), 0, *range(bits + 1, value.ndim))
    return value.reshape(seq_count, requests * owned, *minor)


def merged_over(top, total, sums, seq_count, seq_index):
    reach = 1
    while reach < seq_count:
        half = top.shape[0] // 2
        bit = (seq_index // reach) % 2
        pairs = [(k, k ^ reach) for k in range(seq_count)]

        def chosen(index):
            return [lax.dynamic_slice_in_dim(x, index * half, half, 0) for x in (top, total, sums)]

        sent_top, sent_total, sent_sums = chosen(1 - bit)
        top, total, sums = chosen(bit)
        came_sums = lax.ppermute(sent_sums, "seq", pairs)
        came_top, came_total = lax.ppermute(jnp.stack([sent_top, sent_total]), "seq", pairs)
        common = jnp.maximum(top, came_top)
        own_factor, came_factor = jnp.exp(top - common), jnp.exp(came_top - common)
        top = common
        total = total * own_factor + came_total * came_factor
        sums = sums * own_factor[..., None] + came_sums * came_factor[..., None]
        reach *= 2
    return top, total, sums


def swapped(array):
    return lax.ppermute(array, "batch", [(0, 1), (1, 0)])


def local(
    prompt_cache,
    prompt_states,
    block_steps,
    prompt_lengths,
    target_slots,
    cache_lengths,
    resident_cache,
    token_cache,
    queries,
    resident_states,
    decay_rates,
    step_sizes,
    inner_input,
    inner_gate,
    state_input,
    state_readout,
    skip_gain,
):
    seq_count = lax.axis_size("seq")
    seq_index = lax.axis_index("seq")
    batch_index = lax.axis_index("batch")
    local_prompts, block_len, kv_heads, kv_width = prompt_cache.shape
    head_dim = kv_width // 2
    requests = resident_cache.shape[0]
    channels = decay_rates.shape[1]
    local_channels = channels // seq_count

    own_at = batch_index * local_prompts
    peer_at = (1 - batch_index) * local_prompts
    slot_ids = batch_index * requests + jnp.arange(requests, dtype=jnp.int32)
    matches = target_slots[None, :] == slot_ids[:, None]
    fresh = jnp.any(matches, axis=1)
    chosen_len = jnp.sum(jnp.where(matches, prompt_lengths[None, :], 0), axis=1)
    lengths = jnp.where(fresh, chosen_len, cache_lengths)
    own_match = lax.dynamic_slice_in_dim(matches, own_at, local_prompts, 1)
    peer_match = lax.dynamic_slice_in_dim(matches, peer_at, local_prompts, 1)

    pairs = [(k, k ^ 1) for k in range(seq_count)]
    parity = seq_index % 2
    there = numbers(1 - parity, seq_index * block_len, own_at)
    here = numbers(parity, seq_index * block_len, own_at)
    sent_state, sent_step = pick(
        there, prompt_lengths, prompt_states[:, 0], block_steps, local_channels
    )
    came_state = lax.ppermute(sent_state.astype(jnp.float16), "seq", pairs)
    came_step = lax.ppermute(sent_step, "seq", pairs)
    moved = lax.all_to_all(
        jnp.swapaxes(prompt_cache, 0, 1), "seq", split_axis=0, concat_axis=0, tiled=True
    )
    own_state, own_step = pick(
        here, prompt_lengths, prompt_states[:, 0], block_steps, local_channels
    )
    rates = picked_rates(here, decay_rates, local_channels)
    folded = folded_pair(
        own_state,
        own_step,
        rates,
        came_state.astype(jnp.float32),
        came_step,
        seq_index,
        local_channels,
    )
    handed = hand_over(*folded, rates, local_channels, seq_count // 2, seq_index // 2)

    peer_moved = swapped(moved)
    flat = (block_len, local_prompts, kv_heads * kv_width)
    own_picked = jnp.einsum(
        "rp,ipx->rix",
        own_match.astype(jnp.bfloat16),
        moved.reshape(flat),
        preferred_element_type=jnp.float32,
    )
    picked = own_picked + jnp.einsum(
        "rp,ipx->rix",
        peer_match.astype(jnp.bfloat16),
        peer_moved.reshape(flat),
        preferred_element_type=jnp.float32,
    )
    picked = picked.astype(jnp.bfloat16).reshape(requests, block_len, kv_heads, kv_width)
    position = jnp.arange(block_len, dtype=jnp.int32) * seq_count + seq_index
    merged = jnp.where(fresh[:, None, None, None], picked, resident_cache[:, :, 0])
    merged = jnp.where(
        (position[None, :] < lengths[:, None])[:, :, None, None],
        merged,
        jnp.zeros((), jnp.bfloat16),
    )
    merged = jnp.where(
        (position[None, :] == lengths[:, None])[:, :, None, None], token_cache[:, None], merged
    )
    heads = queries.shape[1]
    group = heads // kv_heads
    grouped = queries.reshape(requests, kv_heads, group, head_dim)
    scores = jnp.einsum(
        "rgqd,rtgd->rgqt", grouped, merged[..., :head_dim], preferred_element_type=jnp.float32
    ) * (1.0 / math.sqrt(head_dim))
    seen = (position[None, :] <= lengths[:, None])[:, None, None, :]
    masked = jnp.where(seen, scores, -1e30)
    highest = jnp.max(masked, axis=3)
    weights = jnp.where(seen, jnp.exp(masked - highest[..., None]), 0.0)
    denominator = jnp.sum(weights, axis=3)
    summed = jnp.einsum(
        "rgqt,rtgd->rgqd",
        weights.astype(jnp.bfloat16),
        merged[..., head_dim:],
        preferred_element_type=jnp.float32,
    )
    owned = heads // seq_count
    part = merged_over(
        owners_first(highest, seq_count, owned),
        owners_first(denominator, seq_count, owned),
        owners_first(summed, seq_count, owned, head_dim),
        seq_count,
        seq_index,
    )
    _, owner_total, owner_sum = part
    attention = (owner_sum[0] / owner_total[0][:, None]).astype(jnp.bfloat16)
    attention = attention.reshape(requests, owned, head_dim)

    rates_here = lax.dynamic_slice_in_dim(
        decay_rates, seq_index * local_channels, local_channels, 1
    )
    peer_handed = swapped(handed)
    chosen_state = jnp.sum(
        jnp.where(own_match[:, :, None, None], handed[None], 0.0), axis=1
    ) + jnp.sum(jnp.where(peer_match[:, :, None, None], peer_handed[None], 0.0), axis=1)
    start = jnp.where(fresh[:, None, None], chosen_state, resident_states)
    inner = inner_input.astype(jnp.float32)
    next_states = (
        jnp.exp(-rates_here[None] * step_sizes[:, None, :]) * start
        + (step_sizes * inner)[:, None, :] * state_input[:, :, None]
    )
    readout = jnp.sum(state_readout[:, :, None] * next_states, axis=1) + skip_gain[None, :] * inner
    mamba_output = (readout * jax.nn.silu(inner_gate.astype(jnp.float32))).astype(jnp.bfloat16)
    return (merged[:, :, None], attention, next_states, mamba_output)


def solution(mesh):
    return jax.shard_map(
        local,
        mesh=mesh,
        in_specs=(
            P(("groups", "batch"), "seq", None, None),
            P(("groups", "batch"), "seq", None, None),
            P(("groups", "batch"), "seq", None),
            P("groups"),
            P("groups"),
            P(("groups", "batch")),
            P(("groups", "batch"), None, "seq", None, None),
            P(("groups", "batch"), None, None),
            P(("groups", "batch"), None, None),
            P(("groups", "batch"), None, "seq"),
            P(),
            P(("groups", "batch"), "seq"),
            P(("groups", "batch"), "seq"),
            P(("groups", "batch"), "seq"),
            P(("groups", "batch"), None),
            P(("groups", "batch"), None),
            P("seq"),
        ),
        out_specs=(
            P(("groups", "batch"), None, "seq", None, None),
            P(("groups", "batch"), "seq", None),
            P(("groups", "batch"), None, "seq"),
            P(("groups", "batch"), "seq"),
        ),
        check_vma=False,
    )
```

```python
import functools
import math

import jax
import jax.numpy as jnp
from jax import lax
from jax.experimental import pallas as pl
from jax.experimental.pallas import tpu as pltpu
from jax.sharding import PartitionSpec as P


STATE_SCALE = 128.0
HALF_SPLIT = 8193.0
KERNEL_VMEM = 8 * 1024 * 1024
PAIRS_A_STEP = 4


def split_half(value):
    spread = value * HALF_SPLIT
    high = spread - (spread - value)
    return high, value - high


def smem():
    return pl.BlockSpec(memory_space=pltpu.SMEM)


def vmem():
    return pl.BlockSpec(memory_space=pltpu.VMEM)


def pick_kernel(flags, usable, state_in, step_in, state_out, step_out, *, width):
    count = state_in.shape[0]
    for q in range(PAIRS_A_STEP):
        source = pl.ds(pl.multiple_of(2 * q * width + flags[0] * width, 128), width)
        target = pl.ds(q * width, width)
        for p in range(count):
            use = usable[p]
            state_out[p, :, target] = state_in[p, :, source] * (use * STATE_SCALE)
            step_out[p : p + 1, target] = step_in[p : p + 1, source] * use


def fold_kernel(
    flags, usable, state_in, step_in, rate_in, came_state, came_step, state_out, step_out, rate_out,
    *, width,
):
    count = state_in.shape[0]
    older = flags[1] == 1
    for q in range(PAIRS_A_STEP):
        source = pl.ds(pl.multiple_of(2 * q * width + flags[0] * width, 128), width)
        target = pl.ds(q * width, width)
        rate = rate_in[:, source]
        rate_out[:, target] = rate
        for p in range(count):
            use = usable[p]
            own = state_in[p, :, source] * (use * STATE_SCALE)
            step = step_in[p : p + 1, source] * use
            came, came_by = came_state[p, :, target], came_step[p : p + 1, target]
            early, late = jnp.where(older, own, came), jnp.where(older, came, own)
            late_by = jnp.where(older, came_by, step)
            state_out[p, :, target] = jnp.exp(-rate * late_by) * early + late
            step_out[p : p + 1, target] = step + came_by


def hop_kernel(
    flags, states, steps, rates, up_in, down_in, up_out, down_out=None, *, width, initial
):
    count, state = states.shape[0], states.shape[1]
    rows = count * state
    up_at = pl.ds(pl.multiple_of(flags[0] * width, 128), width)
    down_at = pl.ds(pl.multiple_of(flags[1] * width, 128), width)
    first, last = flags[2] == 1, flags[3] == 1
    up_wrapped, down_wrapped = flags[4] == 1, flags[5] == 1
    up_rate, down_rate = rates[:, up_at], rates[:, down_at]

    @pl.loop(0, count, unroll=True)
    def _(p):
        here = pl.ds(pl.multiple_of(p * state, state), state)
        there = pl.ds(pl.multiple_of(rows + p * state, state), state)
        wide, narrow = pl.ds(2 * rows + p, 1), pl.ds(2 * rows + count + p, 1)
        own, step = states[p, :, up_at], steps[pl.ds(p, 1), up_at]
        if initial:
            acc, aside, span = own, jnp.zeros_like(own), step
        else:
            high, other = up_in[here, :], up_in[there, :]
            whole = high + other
            acc = jnp.where(first, 0.0, jnp.where(up_wrapped, high, whole))
            acc = jnp.exp(-up_rate * step) * acc + own
            aside = jnp.where(first, whole, other)
            span = up_in[wide, :] + up_in[narrow, :]
            span = jnp.where(up_wrapped, span, span + step)
        high, low = split_half(acc)
        up_out[here, :] = high
        up_out[there, :] = low if initial else jnp.where(up_wrapped, aside, low)
        up_out[wide, :], up_out[narrow, :] = split_half(span)
        if down_out is None:
            return
        own, step = states[p, :, down_at], steps[pl.ds(p, 1), down_at]
        if initial:
            acc, aside, span = own, jnp.zeros_like(own), step
        else:
            high, other = down_in[here, :], down_in[there, :]
            whole = high + other
            span = jnp.where(last, 0.0, down_in[wide, :] + down_in[narrow, :])
            acc = jnp.where(last, 0.0, jnp.where(down_wrapped, high, whole))
            acc = acc + jnp.exp(-down_rate * span) * own
            aside = jnp.where(last, whole, other)
            span = span + step
        high, low = split_half(acc)
        down_out[here, :] = high
        down_out[there, :] = low if initial else jnp.where(down_wrapped, aside, low)
        down_out[wide, :], down_out[narrow, :] = split_half(span)


def last_kernel(flags, states, steps, rates, up_in, down_in, handed, *, width):
    count, state = states.shape[0], states.shape[1]
    rows = count * state
    at = pl.ds(pl.multiple_of(flags[0] * width, 128), width)
    first, last = flags[2] == 1, flags[3] == 1
    up_wrapped, down_wrapped = flags[4] == 1, flags[5] == 1
    rate = rates[:, at]

    @pl.loop(0, count, unroll=True)
    def _(p):
        here = pl.ds(pl.multiple_of(p * state, state), state)
        there = pl.ds(pl.multiple_of(rows + p * state, state), state)
        wide, narrow = pl.ds(2 * rows + p, 1), pl.ds(2 * rows + count + p, 1)
        own, step = states[p, :, at], steps[pl.ds(p, 1), at]
        high, other = up_in[here, :], up_in[there, :]
        whole = high + other
        newest = jnp.where(first, whole, jnp.where(up_wrapped, other, 0.0))
        earlier = jnp.where(first, 0.0, jnp.where(up_wrapped, high, whole))
        span = up_in[wide, :] + up_in[narrow, :]
        high, other = down_in[here, :], down_in[there, :]
        whole = high + other
        oldest = jnp.where(last, whole, jnp.where(down_wrapped, other, 0.0))
        later = jnp.where(last, 0.0, jnp.where(down_wrapped, high, whole))
        span_down = jnp.where(last, 0.0, down_in[wide, :] + down_in[narrow, :])
        outer = jnp.where(up_wrapped, span, 0.0)
        inner = earlier + jnp.exp(-rate * span) * oldest
        inner = later + jnp.exp(-rate * span_down) * (own + jnp.exp(-rate * step) * inner)
        handed[p] = (newest + jnp.exp(-rate * outer) * inner) * (1.0 / STATE_SCALE)


def numbers(*values):
    return jnp.stack([jnp.asarray(v) for v in values]).astype(jnp.int32)


def picked_for_pair(states, steps, usable, seq_index, width):
    count, state, channels = states.shape
    wide = PAIRS_A_STEP * width
    return pl.pallas_call(
        functools.partial(pick_kernel, width=width),
        grid=(channels // (2 * wide),),
        out_shape=(
            jax.ShapeDtypeStruct((count, state, channels // 2), jnp.float32),
            jax.ShapeDtypeStruct((count, channels // 2), jnp.float32),
        ),
        in_specs=[
            smem(),
            smem(),
            pl.BlockSpec((count, state, 2 * wide), lambda n: (0, 0, n)),
            pl.BlockSpec((count, 2 * wide), lambda n: (0, n)),
        ],
        out_specs=(
            pl.BlockSpec((count, state, wide), lambda n: (0, 0, n)),
            pl.BlockSpec((count, wide), lambda n: (0, n)),
        ),
        cost_estimate=pl.CostEstimate(
            flops=states.size, bytes_accessed=6 * states.size, transcendentals=0
        ),
        compiler_params=pltpu.CompilerParams(vmem_limit_bytes=2 * KERNEL_VMEM),
        name="pick_for_pair",
    )(numbers(1 - seq_index % 2), usable, states, steps)


def folded_pair(states, steps, rates, usable, came_state, came_step, seq_index, width):
    count, state, channels = states.shape
    wide = PAIRS_A_STEP * width
    parity = seq_index % 2
    return pl.pallas_call(
        functools.partial(fold_kernel, width=width),
        grid=(channels // (2 * wide),),
        out_shape=(
            jax.ShapeDtypeStruct((count, state, channels // 2), jnp.float32),
            jax.ShapeDtypeStruct((count, channels // 2), jnp.float32),
            jax.ShapeDtypeStruct((state, channels // 2), jnp.float32),
        ),
        in_specs=[
            smem(),
            smem(),
            pl.BlockSpec((count, state, 2 * wide), lambda n: (0, 0, n)),
            pl.BlockSpec((count, 2 * wide), lambda n: (0, n)),
            pl.BlockSpec((state, 2 * wide), lambda n: (0, n)),
            pl.BlockSpec((count, state, wide), lambda n: (0, 0, n)),
            pl.BlockSpec((count, wide), lambda n: (0, n)),
        ],
        out_specs=(
            pl.BlockSpec((count, state, wide), lambda n: (0, 0, n)),
            pl.BlockSpec((count, wide), lambda n: (0, n)),
            pl.BlockSpec((state, wide), lambda n: (0, n)),
        ),
        cost_estimate=pl.CostEstimate(
            flops=4 * states.size, bytes_accessed=10 * states.size, transcendentals=states.size
        ),
        compiler_params=pltpu.CompilerParams(vmem_limit_bytes=2 * KERNEL_VMEM),
        name="fold_pair",
    )(numbers(parity, parity == 0), usable, states, steps, rates, came_state, came_step)


def hand_over(states, steps, rates, width, nodes, node):
    count, state, _ = states.shape
    half = nodes // 2
    ring = 2 * nodes
    ahead = [(k, (k + 2) % ring) for k in range(ring)]
    behind = [(k, (k - 2) % ring) for k in range(ring)]
    rows = 2 * count * state + 2 * count
    payload = jax.ShapeDtypeStruct((rows, width), jnp.float32)
    cost = pl.CostEstimate(
        flops=16 * rows * width, bytes_accessed=16 * rows * width, transcendentals=rows * width
    )
    first, last = node == 0, node == nodes - 1
    up = down = jnp.zeros((8, 128), jnp.float32)
    for hop in range(half):
        both = hop < half - 1
        outs = pl.pallas_call(
            functools.partial(hop_kernel, width=width, initial=hop == 0),
            out_shape=(payload, payload) if both else (payload,),
            in_specs=[smem()] + [vmem()] * 5,
            out_specs=(vmem(), vmem()) if both else (vmem(),),
            cost_estimate=cost,
            compiler_params=pltpu.CompilerParams(vmem_limit_bytes=KERNEL_VMEM),
            name="hop_first" if hop == 0 else "hop_both" if both else "hop_up",
        )(
            numbers(
                (node + half - hop) % nodes,
                (node - (half - 1) + hop) % nodes,
                first,
                last,
                node < hop,
                node + hop >= nodes,
            ),
            states,
            steps,
            rates,
            up,
            down,
        )
        sent = lax.ppermute(outs[0].astype(jnp.float16), "seq", ahead)
        if both:
            down = lax.ppermute(outs[1].astype(jnp.float16), "seq", behind)
            down = down.astype(jnp.float32)
        up = sent.astype(jnp.float32)
    return pl.pallas_call(
        functools.partial(last_kernel, width=width),
        out_shape=jax.ShapeDtypeStruct((count, state, width), jnp.float32),
        in_specs=[smem()] + [vmem()] * 5,
        out_specs=vmem(),
        cost_estimate=cost,
        compiler_params=pltpu.CompilerParams(vmem_limit_bytes=KERNEL_VMEM),
        name="hop_last",
    )(
        numbers(node, node, first, last, node < half, node + half - 1 >= nodes),
        states,
        steps,
        rates,
        up,
        down,
    )


def in_pieces(value):
    pieces = []
    for _ in range(3):
        piece = lax.reduce_precision(value, 5, 10)
        pieces.append(piece)
        value = value - piece
    return jnp.stack(pieces)


def swapped(array):
    return lax.ppermute(array, "batch", [(0, 1), (1, 0)])


def local(
    prompt_cache,
    prompt_states,
    block_steps,
    prompt_lengths,
    target_slots,
    cache_lengths,
    resident_cache,
    token_cache,
    queries,
    resident_states,
    decay_rates,
    step_sizes,
    inner_input,
    inner_gate,
    state_input,
    state_readout,
    skip_gain,
):
    seq_count = lax.axis_size("seq")
    seq_index = lax.axis_index("seq")
    batch_index = lax.axis_index("batch")
    local_prompts, block_len, kv_heads, kv_width = prompt_cache.shape
    head_dim = kv_width // 2
    requests = resident_cache.shape[0]
    channels = decay_rates.shape[1]
    local_channels = channels // seq_count

    own_at = batch_index * local_prompts
    peer_at = (1 - batch_index) * local_prompts
    slot_ids = batch_index * requests + jnp.arange(requests, dtype=jnp.int32)
    matches = target_slots[None, :] == slot_ids[:, None]
    fresh = jnp.any(matches, axis=1)
    chosen_len = jnp.sum(jnp.where(matches, prompt_lengths[None, :], 0), axis=1)
    lengths = jnp.where(fresh, chosen_len, cache_lengths)
    own_match = lax.dynamic_slice_in_dim(matches, own_at, local_prompts, 1)
    peer_match = lax.dynamic_slice_in_dim(matches, peer_at, local_prompts, 1)
    own_lengths = lax.dynamic_slice_in_dim(prompt_lengths, own_at, local_prompts)
    usable = (seq_index * block_len < own_lengths).astype(jnp.float32)

    states, steps = prompt_states[:, 0], block_steps[:, 0]
    pairs = [(k, k ^ 1) for k in range(seq_count)]
    sent_state, sent_step = picked_for_pair(states, steps, usable, seq_index, local_channels)
    came_state = lax.ppermute(sent_state.astype(jnp.float16), "seq", pairs)
    came_step = lax.ppermute(sent_step, "seq", pairs)
    moved = lax.all_to_all(
        jnp.swapaxes(prompt_cache, 0, 1), "seq", split_axis=0, concat_axis=0, tiled=True
    )
    folded = folded_pair(
        states,
        steps,
        decay_rates,
        usable,
        came_state.astype(jnp.float32),
        came_step,
        seq_index,
        local_channels,
    )
    handed = hand_over(*folded, local_channels, seq_count // 2, seq_index // 2)

    peer_moved = swapped(moved)
    flat = (block_len, local_prompts, kv_heads * kv_width)
    own_picked = jnp.einsum(
        "rp,ipx->rix",
        own_match.astype(jnp.bfloat16),
        moved.reshape(flat),
        preferred_element_type=jnp.float32,
    )
    picked = own_picked + jnp.einsum(
        "rp,ipx->rix",
        peer_match.astype(jnp.bfloat16),
        peer_moved.reshape(flat),
        preferred_element_type=jnp.float32,
    )
    picked = picked.astype(jnp.bfloat16).reshape(requests, block_len, kv_heads, kv_width)
    position = jnp.arange(block_len, dtype=jnp.int32) * seq_count + seq_index
    merged = jnp.where(fresh[:, None, None, None], picked, resident_cache[:, :, 0])
    merged = jnp.where(
        (position[None, :] < lengths[:, None])[:, :, None, None],
        merged,
        jnp.zeros((), jnp.bfloat16),
    )
    merged = jnp.where(
        (position[None, :] == lengths[:, None])[:, :, None, None], token_cache[:, None], merged
    )
    heads = queries.shape[1]
    group = heads // kv_heads
    grouped = queries.reshape(requests, kv_heads, group, head_dim)
    scores = jnp.einsum(
        "rgqd,rtgd->rgqt", grouped, merged[..., :head_dim], preferred_element_type=jnp.float32
    ) * (1.0 / math.sqrt(head_dim))
    seen = (position[None, :] <= lengths[:, None])[:, None, None, :]
    masked = jnp.where(seen, scores, -1e30)
    highest = jnp.max(masked, axis=3)
    weights = jnp.where(seen, jnp.exp(masked - highest[..., None]), 0.0)
    denominator = jnp.sum(weights, axis=3)
    summed = jnp.einsum(
        "rgqt,rtgd->rgqd",
        weights.astype(jnp.bfloat16),
        merged[..., head_dim:],
        preferred_element_type=jnp.float32,
    )
    owned = heads // seq_count
    rows = requests * owned
    sums = summed.reshape(requests, seq_count, owned, head_dim)
    sums = jnp.moveaxis(sums, 1, 0).reshape(seq_count, rows, head_dim)
    extra = in_pieces(jnp.stack([highest, denominator])).reshape(6, requests, seq_count, owned)
    extra = jnp.moveaxis(extra, 2, 0).reshape(seq_count, 6 * rows)
    extra = jnp.pad(extra, ((0, 0), (0, head_dim - 6 * rows)))[:, None]
    parcels = lax.all_to_all(
        jnp.concatenate([sums, extra], axis=1).astype(jnp.float16),
        "seq",
        split_axis=0,
        concat_axis=0,
        tiled=True,
    ).astype(jnp.float32)
    peer_sum = parcels[:, :rows]
    peer_extra = parcels[:, rows, : 6 * rows].reshape(seq_count, 3, 2, rows)
    peer_extra = (peer_extra[:, 2] + peer_extra[:, 1]) + peer_extra[:, 0]
    peer_top, peer_total = peer_extra[:, 0], peer_extra[:, 1]
    common_top = jnp.max(peer_top, axis=0)
    factor = jnp.exp(peer_top - common_top[None])
    owner_total = jnp.sum(peer_total * factor, axis=0)
    owner_sum = jnp.sum(peer_sum * factor[..., None], axis=0)
    attention = (owner_sum / owner_total[..., None]).astype(jnp.bfloat16)
    attention = attention.reshape(requests, owned, head_dim)

    rates_here = lax.dynamic_slice_in_dim(
        decay_rates, seq_index * local_channels, local_channels, 1
    )
    peer_handed = swapped(handed)
    chosen_state = jnp.sum(
        jnp.where(own_match[:, :, None, None], handed[None], 0.0), axis=1
    ) + jnp.sum(jnp.where(peer_match[:, :, None, None], peer_handed[None], 0.0), axis=1)
    start = jnp.where(fresh[:, None, None], chosen_state, resident_states)
    inner = inner_input.astype(jnp.float32)
    next_states = (
        jnp.exp(-rates_here[None] * step_sizes[:, None, :]) * start
        + (step_sizes * inner)[:, None, :] * state_input[:, :, None]
    )
    readout = jnp.sum(state_readout[:, :, None] * next_states, axis=1) + skip_gain[None, :] * inner
    mamba_output = (readout * jax.nn.silu(inner_gate.astype(jnp.float32))).astype(jnp.bfloat16)
    return (merged[:, :, None], attention, next_states, mamba_output)


def solution(mesh):
    return jax.shard_map(
        local,
        mesh=mesh,
        in_specs=(
            P(("groups", "batch"), "seq", None, None),
            P(("groups", "batch"), "seq", None, None),
            P(("groups", "batch"), "seq", None),
            P("groups"),
            P("groups"),
            P(("groups", "batch")),
            P(("groups", "batch"), None, "seq", None, None),
            P(("groups", "batch"), None, None),
            P(("groups", "batch"), None, None),
            P(("groups", "batch"), None, "seq"),
            P(),
            P(("groups", "batch"), "seq"),
            P(("groups", "batch"), "seq"),
            P(("groups", "batch"), "seq"),
            P(("groups", "batch"), None),
            P(("groups", "batch"), None),
            P("seq"),
        ),
        out_specs=(
            P(("groups", "batch"), None, "seq", None, None),
            P(("groups", "batch"), "seq", None),
            P(("groups", "batch"), None, "seq"),
            P(("groups", "batch"), "seq"),
        ),
        check_vma=False,
    )
```
